256 devices in a mesh: pair: 4 (over z_lo, core), dp: 64 (over z_hi, x, y).
Axes of the slice: x: 4, y: 4, z: 8 (z_hi: 4, z_lo: 2; z = z_hi * 2 + z_lo), core: 2. Of those that a mesh axis runs over, the one named last changes fastest.
Arguments:
- master: float32 [4, 1048576], P('pair', 'dp'), may hold values from -6 to 6
- moment1: float32 [4, 1048576], P('pair', 'dp'), may hold values from -4 to 4
- moment2: float32 [4, 1048576], P('pair', 'dp'), may hold values from 0.05 to 2
- local_grad: bfloat16 [4, 64, 1048576], P('pair', 'dp'), may hold values from -16 to 16
- partner: int32 [64, 4], P('dp'), may hold values from 0 to 3, as said below
Outputs:
- new_master: float32 [4, 64, 2, 16384], P('pair', 'dp')
- new_moment1: float32 [4, 64, 2, 16384], P('pair', 'dp')
- new_moment2: float32 [4, 64, 2, 16384], P('pair', 'dp')
The draws below stay inside these ranges and needn't reach their ends.
Inputs may be any that keep to these rules, and one draw needn't show every extreme that they name: partner[d, partner[d, i]] == i and partner[d, i] != i for every d and i: each row a perfect matching of the 4 pair indices.
All inputs are finite; a program needn't handle non-finite values.
Results may differ from the reference program's by a relative error of at most 0.0003.
Values sent between devices are 32-bit elements; how exact they have to be, the bound alone decides.
A program may use at most 64 MiB of HBM per device.

```python
import math
import jax
import jax.numpy as jnp
from jax import lax

SH = 16384
NSH = 1048576
N_PAIR = 4
N_DP = 64


def draw_partner(key, part):
    xor_masks = jax.random.randint(key, (N_DP, 1), 1, 4, dtype=jnp.int32)
    return jnp.bitwise_xor(jnp.arange(N_PAIR, dtype=jnp.int32)[None, :], xor_masks)


def with_spikes(entries, own_key, source, target, shards_of, factor):
    owner, partner = [(jnp.arange(entries.shape[dim]) // (entries.shape[dim] // shards_of)).reshape([-1 if axis == dim else 1 for axis in range(entries.ndim)]) for dim in (source, target)]
    chosen = jax.random.permutation(own_key, shards_of)[partner]
    strong = (owner == chosen) | (owner == (partner + shards_of // 2) % shards_of)
    return jnp.where(strong, factor * entries, entries)


def shard_levels(rng, dims, cuts, least, largest):
    def one(axis_at, shards_of):
        draws = jax.random.uniform(jax.random.fold_in(jax.random.fold_in(rng, 6), axis_at), (shards_of,), jnp.float32, least / len(cuts), largest / len(cuts))
        return jnp.repeat(jnp.exp(draws), dims[axis_at] // shards_of).reshape((-1,) + (1,) * (len(dims) - axis_at - 1))

    loudness = one(*cuts[0])
    for cut in cuts[1:]:
        loudness = loudness * one(*cut)
    return loudness


def scatter_about(rng, dims, scale, reach, split=(), kind=jnp.bfloat16):
    result = jax.random.normal(rng, dims, jnp.float32) * scale
    if len(split) > 0:
        result = shard_levels(rng, dims, split, -0.22, 0.18) * result
    return jnp.clip(result, min=-reach, max=reach).astype(kind)


def noise_with(stream_key, shape, deviation, most, shards, heavy, held_as=jnp.bfloat16):
    entries = deviation * jax.random.normal(stream_key, shape, jnp.float32)
    if shards:
        entries = entries * shard_levels(stream_key, shape, shards, -0.22, 0.18)
    return jnp.clip(with_spikes(entries, jax.random.fold_in(stream_key, 3), *heavy), -most, most).astype(held_as)


def setup_inputs(seed: int = 0) -> dict:
    streams_of = jax.random.split(jax.random.key(seed), 6)
    master = scatter_about(streams_of[0], (N_PAIR, NSH), 1.0, 6.0, ((0, 4), (1, 64)), jnp.float32)
    moment1 = scatter_about(streams_of[1], (N_PAIR, NSH), 0.5, 4.0, ((0, 4), (1, 64)), jnp.float32)
    moment2 = jnp.clip(jnp.exp(math.log(2.0) - 3.6888794 * jax.random.uniform(streams_of[2], (N_PAIR, NSH), jnp.float32) ** shard_levels(streams_of[2], (N_PAIR, NSH), ((0, 4), (1, 64)), -0.2, 0.2)), 0.05, 2.0)
    local_grad = noise_with(streams_of[3], (N_PAIR, N_DP, NSH), 1.0, 16.0, ((0, 4), (1, 64)), (1, 2, 64, 4.0))
    partner = draw_partner(jax.random.fold_in(streams_of[5], 71), 0)
    return dict(master=master, moment1=moment1, moment2=moment2, local_grad=local_grad, partner=partner)


beta_one = 0.9
beta_two = 0.95
bias_one = 1.0 - 0.9 ** 10
bias_two = 1.0 - 0.95 ** 10
rate = 0.001
decay = 0.1
eps_value = 1e-08

def adamw_update(weights, first, second, grads, scale):
    scaled = scale * grads
    first_new = beta_one * first + (1.0 - beta_one) * scaled
    second_new = beta_two * second + (1.0 - beta_two) * scaled * scaled
    change = first_new / bias_one / (jnp.sqrt(second_new / bias_two) + eps_value) + decay * weights
    return (weights - rate * change, first_new, second_new)

def reference(master, moment1, moment2, local_grad, partner):
    n_pair = master.shape[0]
    columns = master.shape[1]

    def add_block(index, running):
        return running + lax.dynamic_index_in_dim(local_grad, index, 1, keepdims=False).astype(jnp.float32)
    total = lax.fori_loop(0, N_DP, add_block, jnp.zeros((n_pair, columns), jnp.float32))
    norm2 = jnp.sum(total * total)
    scale = 1.0 / jnp.maximum(jnp.sqrt(norm2 / (n_pair * columns)), 1.0)
    weights, first, second = adamw_update(master, moment1, moment2, total, scale)
    owners = jnp.arange(n_pair, dtype=jnp.int32)
    mates = jnp.transpose(partner).astype(jnp.int32)
    survive = owners[:, None] < mates

    def arrange(values):
        blocks = values.reshape(n_pair, N_DP, SH)
        other = jnp.take_along_axis(blocks, mates[:, :, None], axis=0)
        paired = jnp.stack([blocks, other], axis=2)
        return jnp.where(survive[:, :, None, None], paired, 0.0)
    return (arrange(weights), arrange(first), arrange(second))
```

```python
import functools

import jax
import jax.numpy as jnp
from jax import lax
from jax.experimental import pallas as pl
from jax.experimental.pallas import tpu as pltpu
from jax.sharding import Mesh
from jax.sharding import PartitionSpec as P

beta_one = 0.9
beta_two = 0.95
bias_one = 1.0 - 0.9**10
bias_two = 1.0 - 0.95**10
rate = 0.001
decay = 0.1
eps_value = 1e-08

SH = 16384
N_DP = 64
PAIR = ("zl", "core")
DP = ("zh", "x", "y")
STRIDE = {"zh": 16, "x": 4, "y": 1}
MESH = pl.DeviceIdType.MESH

PARTS = (
    (("x", "y", "zh"), 0, 56, 32),
    (("y", "x", "zh"), 56, 56, 32),
    (("zh", "x", "y"), 112, 16, 8),
)
FIRST = (2, 0, 1)
AP, AM, BP, BM, CP, CM = range(6)


def kernel(
    partner, w_hbm, m_hbm, v_hbm, g_hbm, out_w, out_m, out_v,
    stage, own, cand, grads, cand_g, near, far,
    f0, f1, f2, r0, r1, r2, s0, s1, s2, q0, q1, q2, t0, t1, t2, u0, u1, u2,
    load_sem, own_sem, ring_send, ring_recv, pair_send, pair_recv, near_send, near_recv, far_send, far_recv,
):
    data = ((f0, s0, t0), (f1, s1, t1), (f2, s2, t2))
    landing = ((r0, q0, u0), (r1, q1, u1), (r2, q2, u2))
    at = {a: lax.axis_index(a) for a in PAIR + DP}

    def beside(axis, step):
        return lax.rem(at[axis] + step + 4, 4)

    loads = [
        pltpu.make_async_copy(
            g_hbm.at[0, :, pl.ds(i * (N_DP // 4) * SH, (N_DP // 4) * SH)],
            stage.at[:, pl.ds(i * (N_DP // 4) * SH, (N_DP // 4) * SH)],
            load_sem.at[i],
        )
        for i in range(4)
    ]
    owns = [pltpu.make_async_copy(ref, own.at[i], own_sem.at[i]) for i, ref in enumerate((w_hbm, m_hbm, v_hbm))]
    for c in loads + owns:
        c.start()
    barrier = pltpu.get_barrier_semaphore()
    near_ids = [
        {"zh": beside("zh", k // 4), "zl": lax.rem(at["zl"] + (k // 2) % 2, 2), "core": lax.rem(at["core"] + k % 2, 2)}
        for k in range(16)
    ]
    far_ids = [{"x": beside("x", k // 4), "y": beside("y", k % 4)} for k in range(16)]
    for k in range(1, 16):
        pl.semaphore_signal(barrier, inc=1, device_id=near_ids[k], device_id_type=MESH)
        pl.semaphore_signal(barrier, inc=1, device_id=far_ids[k], device_id_type=MESH)

    def convert(part, c0, half):
        order, row, rows, _ = PARTS[part]
        dst = data[part][0]

        def body(i, carry):
            c1 = half * 2 + i // 4
            c2 = lax.rem(i, 4)
            block = c0 * STRIDE[order[0]] + c1 * STRIDE[order[1]] + c2 * STRIDE[order[2]]
            for j in range(rows // 8):
                piece = stage[0:1, pl.ds(pl.multiple_of(block * SH + (row + 8 * j) * 128, 1024), 1024)]
                dst[c0, c1, c2, pl.ds(8 * j, 8), :] = piece.astype(jnp.float32).reshape(8, 128)
            return carry

        lax.fori_loop(0, 8, body, 0)

    def view(part, phase, c, half):
        ref = data[part][phase]
        if phase < 2:
            return ref.at[c, pl.ds(2 * half, 2)]
        cut, rows = PARTS[part][3], PARTS[part][2]
        return ref.at[c, pl.ds(0, cut)] if half == 0 else ref.at[c, pl.ds(cut, rows - cut)]

    def landed(part, phase, kind, half):
        ref = landing[part][phase].at[kind]
        if phase < 2:
            return ref
        cut, rows = PARTS[part][3], PARTS[part][2]
        return ref.at[pl.ds(0, cut if half == 0 else rows - cut)]

    HALF = {AP: 0, AM: 1, BP: 1, BM: 0, CP: 0, CM: 1}
    CHUNK = {AP: 2, AM: -2, BP: 1, BM: -1, CP: 1, CM: -1}

    def ring(part, phase, kind):
        axis = PARTS[part][0][phase]
        n = (part * 3 + phase) * 6 + kind
        return pltpu.make_async_remote_copy(
            src_ref=view(part, phase, beside(axis, CHUNK[kind]), HALF[kind]),
            dst_ref=landed(part, phase, kind, HALF[kind]),
            send_sem=ring_send.at[n],
            recv_sem=ring_recv.at[n],
            device_id={axis: beside(axis, 1 if kind in (AP, BP, CP) else -1)},
            device_id_type=MESH,
        )

    def flat(ref):
        shape = ref.shape
        rows = shape[-2] // 8
        lead = [()]
        for n in shape[:-2]:
            lead = [i + (j,) for i in lead for j in range(n)]
        return lead, rows

    def add_up(dst, *srcs):
        lead, rows = flat(dst)
        if len(lead) > 2:
            n1 = dst.shape[1]

            def body(i, carry):
                idx = (i // n1, lax.rem(i, n1))
                for j in range(rows):
                    tile = idx + (pl.ds(8 * j, 8), slice(None))
                    total = srcs[0][tile]
                    for s in srcs[1:]:
                        total = total + s[tile]
                    dst[tile] = total
                return carry

            lax.fori_loop(0, len(lead), body, 0)
        else:
            for idx in lead:
                for j in range(rows):
                    tile = idx + (pl.ds(8 * j, 8), slice(None))
                    total = srcs[0][tile]
                    for s in srcs[1:]:
                        total = total + s[tile]
                    dst[tile] = total

    def open_phase(part, phase):
        for kind in (AP, AM, BP, BM):
            ring(part, phase, kind).start()

    def forward(part, phase):
        axis = PARTS[part][0][phase]
        for a, c in ((AP, CP), (AM, CM)):
            ring(part, phase, a).wait_recv()
            mine = view(part, phase, beside(axis, CHUNK[c]), HALF[c])
            add_up(mine, mine, landed(part, phase, a, HALF[a]))
            ring(part, phase, c).start()

    def close_phase(part, phase):
        axis = PARTS[part][0][phase]
        for kind in (BP, BM, CP, CM):
            ring(part, phase, kind).wait_recv()
        for half, b, c in ((0, BM, CP), (1, BP, CM)):
            srcs = (
                view(part, phase, at[axis], half),
                landed(part, phase, b, half),
                landed(part, phase, c, half),
            )
            if phase < 2:
                add_up(data[part][phase + 1].at[pl.ds(2 * half, 2)], *srcs)
            else:
                row, rows, cut = PARTS[part][1:]
                lo, n = (0, cut) if half == 0 else (cut, rows - cut)
                add_up(grads.at[pl.ds(row + lo, n)], *srcs)

    for c in loads:
        c.wait()
    for part in FIRST:
        axis = PARTS[part][0][0]
        convert(part, beside(axis, 2), 0)
        convert(part, beside(axis, 2), 1)
    pl.semaphore_wait(barrier, 30)
    for part in FIRST:
        ring(part, 0, AP).start()
        ring(part, 0, AM).start()
    for part in FIRST:
        axis = PARTS[part][0][0]
        convert(part, beside(axis, 1), 1)
        convert(part, beside(axis, -1), 0)
        ring(part, 0, BP).start()
        ring(part, 0, BM).start()
    for part in FIRST:
        axis = PARTS[part][0][0]
        convert(part, beside(axis, 1), 0)
        convert(part, beside(axis, -1), 1)
        convert(part, at[axis], 0)
        convert(part, at[axis], 1)
    for part in FIRST:
        forward(part, 0)

    def pair_copy(src, dst, n, axis):
        return pltpu.make_async_remote_copy(
            src_ref=src, dst_ref=dst, send_sem=pair_send.at[n], recv_sem=pair_recv.at[n],
            device_id={axis: 1 - at[axis]}, device_id_type=MESH,
        )

    for c in owns:
        c.wait()
    shard_1 = pair_copy(own, cand.at[0], 0, "core")
    shard_2 = pair_copy(own, cand.at[1], 1, "zl")
    shard_3 = pair_copy(cand.at[1], cand.at[2], 2, "core")
    shard_1.start()
    shard_2.start()

    for phase in (0, 1, 2):
        for part in FIRST:
            close_phase(part, phase)
            if phase < 2:
                open_phase(part, phase + 1)
        if phase < 2:
            for part in FIRST:
                forward(part, phase + 1)
        if phase == 0:
            shard_2.wait_recv()
            shard_3.start()

    def squares(i, total):
        tile = grads[pl.ds(pl.multiple_of(i * 8, 8), 8), :]
        return total + tile * tile

    total = lax.fori_loop(0, 16, squares, jnp.zeros((8, 128), jnp.float32))
    near[0] = jnp.sum(total, axis=0, keepdims=True)

    def spread(buf, k, ids, send, recv):
        return pltpu.make_async_remote_copy(
            src_ref=buf.at[0], dst_ref=buf.at[k], send_sem=send.at[k], recv_sem=recv.at[k],
            device_id=ids[k], device_id_type=MESH,
        )

    near_copies = [spread(near, k, near_ids, near_send, near_recv) for k in range(1, 16)]
    far_copies = [spread(far, k, far_ids, far_send, far_recv) for k in range(1, 16)]
    grads_1 = pair_copy(grads, cand_g.at[0], 3, "core")
    grads_2 = pair_copy(grads, cand_g.at[1], 4, "zl")
    grads_3 = pair_copy(cand_g.at[1], cand_g.at[2], 5, "core")
    for c in near_copies:
        c.start()
    grads_1.start()
    grads_2.start()
    for c in near_copies:
        c.wait_recv()
    far[0] = functools.reduce(jnp.add, [near[k] for k in range(16)])
    for c in far_copies:
        c.start()
    grads_2.wait_recv()
    grads_3.start()
    for c in far_copies:
        c.wait_recv()
    norm2 = jnp.sum(functools.reduce(jnp.add, [far[k] for k in range(16)]), axis=1, keepdims=True)
    scale = 1.0 / jnp.maximum(jnp.sqrt(norm2 / (4 * N_DP * SH)), 1.0)

    shard_1.wait_recv()
    shard_3.wait_recv()
    grads_1.wait_recv()
    grads_3.wait_recv()
    mine = at["zl"] * 2 + at["core"]
    mate = partner[0, mine]
    apart = jnp.full((1, 1024), mine ^ mate, jnp.int32)
    is_one, is_two = apart == 1, apart == 2
    survive = jnp.full((1, 1024), mate - mine, jnp.int32) > 0

    def update(i, carry):
        cols = pl.ds(pl.multiple_of(i * 1024, 1024), 1024)
        rows = pl.ds(pl.multiple_of(i * 8, 8), 8)

        def chosen(one, two, three):
            return jnp.where(is_one, one, jnp.where(is_two, two, three))

        for slot in (0, 1):
            if slot == 0:
                weights, first, second = [own[a, :, cols] for a in range(3)]
                total = grads[rows, :].reshape(1, 1024)
            else:
                weights, first, second = [chosen(*[cand[k, a, :, cols] for k in range(3)]) for a in range(3)]
                total = chosen(*[cand_g[k, rows, :].reshape(1, 1024) for k in range(3)])
            scaled = scale * total
            first_new = beta_one * first + (1.0 - beta_one) * scaled
            second_new = beta_two * second + (1.0 - beta_two) * scaled * scaled
            change = first_new / bias_one / (jnp.sqrt(second_new / bias_two) + eps_value) + decay * weights
            for ref, value in ((out_w, weights - rate * change), (out_m, first_new), (out_v, second_new)):
                ref[0, 0, slot : slot + 1, cols] = jnp.where(survive, value, 0.0)
        return carry

    lax.fori_loop(0, 16, update, 0)

    for part in range(3):
        for phase in range(3):
            for kind in range(6):
                ring(part, phase, kind).wait_send()
    for c in [shard_1, shard_2, shard_3, grads_1, grads_2, grads_3] + near_copies + far_copies:
        c.wait_send()


def on_device(master, moment1, moment2, local_grad, partner):
    f32 = jnp.float32
    vmem = [pltpu.VMEM((4, 4, 4, p[2], 128), f32) for p in PARTS]
    vmem += [pltpu.VMEM((6, 2, 4, p[2], 128), f32) for p in PARTS]
    vmem += [pltpu.VMEM((4, 4, p[2], 128), f32) for p in PARTS]
    vmem += [pltpu.VMEM((6, 2, p[2], 128), f32) for p in PARTS]
    vmem += [pltpu.VMEM((4, p[2], 128), f32) for p in PARTS]
    vmem += [pltpu.VMEM((6, p[3], 128), f32) for p in PARTS]
    dma = pltpu.SemaphoreType.DMA
    out = jax.ShapeDtypeStruct((1, 1, 2, SH), f32)
    return pl.pallas_call(
        kernel,
        out_shape=(out, out, out),
        in_specs=[pl.BlockSpec(memory_space=pltpu.SMEM)] + [pl.BlockSpec(memory_space=pltpu.HBM)] * 4,
        out_specs=[pl.BlockSpec(memory_space=pltpu.VMEM)] * 3,
        scratch_shapes=[
            pltpu.VMEM((1, N_DP * SH), jnp.bfloat16),
            pltpu.VMEM((3, 1, SH), f32),
            pltpu.VMEM((3, 3, 1, SH), f32),
            pltpu.VMEM((128, 128), f32),
            pltpu.VMEM((3, 128, 128), f32),
            pltpu.VMEM((16, 1, 128), f32),
            pltpu.VMEM((16, 1, 128), f32),
        ]
        + vmem
        + [dma((4,)), dma((3,)), dma((54,)), dma((54,)), dma((6,)), dma((6,))]
        + [dma((16,))] * 4,
        compiler_params=pltpu.CompilerParams(collective_id=0, has_side_effects=True),
        name="step",
    )(partner, master, moment1, moment2, local_grad)


def solution(mesh):
    finer = Mesh(mesh.devices.reshape(2, 2, 4, 4, 4), PAIR + DP)
    in_specs = (P(PAIR, DP), P(PAIR, DP), P(PAIR, DP), P(PAIR, DP, None), P(DP, None))
    out_specs = (P(PAIR, DP, None, None),) * 3
    return jax.shard_map(on_device, mesh=finer, in_specs=in_specs, out_specs=out_specs, check_vma=False)
```

```python
import functools

import jax
import jax.numpy as jnp
from jax import lax
from jax.experimental import pallas as pl
from jax.experimental.pallas import tpu as pltpu
from jax.sharding import Mesh
from jax.sharding import PartitionSpec as P

beta_one = 0.9
beta_two = 0.95
bias_one = 1.0 - 0.9**10
bias_two = 1.0 - 0.95**10
rate = 0.001
decay = 0.1
eps_value = 1e-08

SH = 16384
N_DP = 64
PAIR = ("zl", "core")
DP = ("zh", "x", "y")
STRIDE = {"zh": 16, "x": 4, "y": 1}
MESH = pl.DeviceIdType.MESH

PARTS = (
    (("x", "y", "zh"), 0, 56, 32),
    (("y", "x", "zh"), 56, 56, 32),
    (("zh", "x", "y"), 112, 16, 8),
)
FIRST = (2, 0, 1)
AP, AM, BP, BM, CP, CM = range(6)


def kernel(
    partner, w_hbm, m_hbm, v_hbm, g_hbm, state, squares_sum,
    stage, own, cand, grads, cand_g, near, far,
    f0, f1, f2, r0, r1, r2, s0, s1, s2, q0, q1, q2, t0, t1, t2, u0, u1, u2,
    load_sem, own_sem, ring_send, ring_recv, pair_send, pair_recv, norm_send, norm_recv,
):
    data = ((f0, s0, t0), (f1, s1, t1), (f2, s2, t2))
    landing = ((r0, q0, u0), (r1, q1, u1), (r2, q2, u2))
    at = {a: lax.axis_index(a) for a in PAIR + DP}

    def beside(axis, step):
        return lax.rem(at[axis] + step + 4, 4)

    groups = (2, 1, -1, 0)
    for i in groups:
        for zh in range(4):
            cols = pl.ds((zh * 16 + beside("x", i) * 4) * SH, 4 * SH)
            pltpu.make_async_copy(g_hbm.at[0, :, cols], stage.at[:, cols], load_sem.at[i % 4]).start()
    for i, ref in enumerate((w_hbm, m_hbm, v_hbm)):
        pltpu.make_async_copy(ref, own.at[i], own_sem).start()

    def loaded(i):
        part_of = stage.at[:, pl.ds(0, 16 * SH)]
        pltpu.make_async_copy(part_of, part_of, load_sem.at[i % 4]).wait()

    barrier = pltpu.get_barrier_semaphore()
    near_ids = [
        {"zh": beside("zh", k // 4), "zl": lax.rem(at["zl"] + (k // 2) % 2, 2), "core": lax.rem(at["core"] + k % 2, 2)}
        for k in range(16)
    ]
    far_ids = [{"x": beside("x", k // 4), "y": beside("y", k % 4)} for k in range(16)]
    for k in range(1, 16):
        pl.semaphore_signal(barrier, inc=1, device_id=near_ids[k], device_id_type=MESH)
        pl.semaphore_signal(barrier, inc=1, device_id=far_ids[k], device_id_type=MESH)

    def convert(part, c0, half):
        order, row, rows, _ = PARTS[part]
        dst = data[part][0]

        def body(i, carry):
            c1 = half * 2 + i // 4
            c2 = lax.rem(i, 4)
            block = c0 * STRIDE[order[0]] + c1 * STRIDE[order[1]] + c2 * STRIDE[order[2]]
            for j in range(rows // 8):
                piece = stage[0:1, pl.ds(pl.multiple_of(block * SH + (row + 8 * j) * 128, 1024), 1024)]
                dst[c0, c1, c2, pl.ds(8 * j, 8), :] = piece.astype(jnp.float32).reshape(8, 128)
            return carry

        lax.fori_loop(0, 8, body, 0)

    def view(part, phase, c, half):
        ref = data[part][phase]
        if phase < 2:
            return ref.at[c, pl.ds(2 * half, 2)]
        cut, rows = PARTS[part][3], PARTS[part][2]
        return ref.at[c, pl.ds(0, cut)] if half == 0 else ref.at[c, pl.ds(cut, rows - cut)]

    def landed(part, phase, kind, half):
        ref = landing[part][phase].at[kind]
        if phase < 2:
            return ref
        cut, rows = PARTS[part][3], PARTS[part][2]
        return ref.at[pl.ds(0, cut if half == 0 else rows - cut)]

    HALF = {AP: 0, AM: 1, BP: 1, BM: 0, CP: 0, CM: 1}
    CHUNK = {AP: 2, AM: -2, BP: 1, BM: -1, CP: 1, CM: -1}

    def ring(part, phase, kind):
        axis = PARTS[part][0][phase]
        n = part * 3 + phase
        return pltpu.make_async_remote_copy(
            src_ref=view(part, phase, beside(axis, CHUNK[kind]), HALF[kind]),
            dst_ref=landed(part, phase, kind, HALF[kind]),
            send_sem=ring_send.at[n],
            recv_sem=ring_recv.at[n * 3 + min(kind, BP)],
            device_id={axis: beside(axis, 1 if kind in (AP, BP, CP) else -1)},
            device_id_type=MESH,
        )

    def wait_bytes(ref, sem):
        pltpu.make_async_copy(ref, ref, sem).wait()

    def flat(ref):
        shape = ref.shape
        rows = shape[-2] // 8
        lead = [()]
        for n in shape[:-2]:
            lead = [i + (j,) for i in lead for j in range(n)]
        return lead, rows

    def add_up(dst, *srcs):
        lead, rows = flat(dst)
        if len(lead) > 2:
            n1 = dst.shape[1]

            def body(i, carry):
                idx = (i // n1, lax.rem(i, n1))
                for j in range(rows):
                    tile = idx + (pl.ds(8 * j, 8), slice(None))
                    total = srcs[0][tile]
                    for s in srcs[1:]:
                        total = total + s[tile]
                    dst[tile] = total
                return carry

            lax.fori_loop(0, len(lead), body, 0)
        else:
            for idx in lead:
                for j in range(rows):
                    tile = idx + (pl.ds(8 * j, 8), slice(None))
                    total = srcs[0][tile]
                    for s in srcs[1:]:
                        total = total + s[tile]
                    dst[tile] = total

    def open_phase(part, phase):
        for kind in (AP, AM, BP, BM):
            ring(part, phase, kind).start()

    def forward(part, phase):
        axis = PARTS[part][0][phase]
        for a, c in ((AP, CP), (AM, CM)):
            ring(part, phase, a).wait_recv()
            mine = view(part, phase, beside(axis, CHUNK[c]), HALF[c])
            add_up(mine, mine, landed(part, phase, a, HALF[a]))
            ring(part, phase, c).start()

    def close_phase(part, phase):
        axis = PARTS[part][0][phase]
        last = data[part][2].at[pl.ds(0, 2)]
        wait_bytes(last if phase == 2 else landing[part][phase].at[pl.ds(2, 4)], ring_recv.at[(part * 3 + phase) * 3 + BP])
        for half, b, c in ((0, BM, CP), (1, BP, CM)):
            srcs = (
                view(part, phase, at[axis], half),
                landed(part, phase, b, half),
                landed(part, phase, c, half),
            )
            if phase < 2:
                add_up(data[part][phase + 1].at[pl.ds(2 * half, 2)], *srcs)
            else:
                row, rows, cut = PARTS[part][1:]
                lo, n = (0, cut) if half == 0 else (cut, rows - cut)
                add_up(grads.at[pl.ds(row + lo, n)], *srcs)

    for part in (0, 1, 2):
        axis = PARTS[part][0][0]
        for i in groups[:1] if part == 0 else groups[1:] if part == 1 else ():
            loaded(i)
        convert(part, beside(axis, 2), 0)
        convert(part, beside(axis, 2), 1)
        if part == 0:
            pl.semaphore_wait(barrier, 30)
        ring(part, 0, AP).start()
        ring(part, 0, AM).start()
    for part in (0, 1, 2):
        axis = PARTS[part][0][0]
        convert(part, beside(axis, 1), 1)
        convert(part, beside(axis, -1), 0)
        ring(part, 0, BP).start()
        ring(part, 0, BM).start()
    for part in FIRST:
        axis = PARTS[part][0][0]
        convert(part, beside(axis, 1), 0)
        convert(part, beside(axis, -1), 1)
        convert(part, at[axis], 0)
        convert(part, at[axis], 1)
    for part in FIRST:
        forward(part, 0)

    def pair_copy(src, dst, n, axis):
        return pltpu.make_async_remote_copy(
            src_ref=src, dst_ref=dst, send_sem=pair_send.at[n // 2], recv_sem=pair_recv.at[n],
            device_id={axis: 1 - at[axis]}, device_id_type=MESH,
        )

    wait_bytes(own, own_sem)
    shard_1 = pair_copy(own, cand.at[0], 0, "core")
    shard_2 = pair_copy(own, cand.at[2], 1, "zl")
    shard_3 = pair_copy(cand.at[2], cand.at[1], 0, "core")
    shard_1.start()
    shard_2.start()

    mine = at["zl"] * 2 + at["core"]
    mate = partner[0, mine]
    apart = jnp.full((1, 1024), mine ^ mate, jnp.int32)
    is_one, is_two = apart == 1, apart == 2
    survive = jnp.full((1, 1024), mate - mine, jnp.int32) > 0

    def keep(a, cols, value, values):
        theirs = jnp.where(is_one, values[0], jnp.where(is_two, values[1], values[2]))
        state[a, 0:1, cols] = jnp.where(survive, value, 0.0)
        state[a, 1:2, cols] = jnp.where(survive, theirs, 0.0)

    def choose(i, carry):
        cols = pl.ds(pl.multiple_of(i * 1024, 1024), 1024)
        for a in range(3):
            keep(a, cols, own[a, :, cols], [cand[k, a, :, cols] for k in (0, 2, 1)])
        return carry

    def choose_grads(i, carry):
        cols = pl.ds(pl.multiple_of(i * 1024, 1024), 1024)
        rows = pl.ds(pl.multiple_of(i * 8, 8), 8)
        keep(3, cols, grads[rows, :].reshape(1, 1024), [cand_g[k, rows, :].reshape(1, 1024) for k in (0, 2, 1)])
        return carry

    for phase in (0, 1, 2):
        for part in FIRST:
            close_phase(part, phase)
            if phase < 2:
                open_phase(part, phase + 1)
        if phase < 2:
            for part in FIRST:
                forward(part, phase + 1)
        if phase == 0:
            shard_2.wait_recv()
            shard_3.start()
        if phase == 1:
            wait_bytes(cand.at[pl.ds(0, 2)], pair_recv.at[0])
            lax.fori_loop(0, 16, choose, 0)

    def squares(i, total):
        tile = grads[pl.ds(pl.multiple_of(i * 8, 8), 8), :]
        return total + tile * tile

    total = lax.fori_loop(0, 16, squares, jnp.zeros((8, 128), jnp.float32))
    near[0] = jnp.sum(total, axis=0, keepdims=True)

    def spread(buf, k, ids, n):
        return pltpu.make_async_remote_copy(
            src_ref=buf.at[0], dst_ref=buf.at[k], send_sem=norm_send.at[n], recv_sem=norm_recv.at[n],
            device_id=ids[k], device_id_type=MESH,
        )

    grads_1 = pair_copy(grads, cand_g.at[0], 2, "core")
    grads_2 = pair_copy(grads, cand_g.at[2], 3, "zl")
    grads_3 = pair_copy(cand_g.at[2], cand_g.at[1], 2, "core")
    for k in range(1, 16):
        spread(near, k, near_ids, 0).start()
    grads_1.start()
    grads_2.start()
    wait_bytes(near.at[pl.ds(1, 15)], norm_recv.at[0])
    far[0] = functools.reduce(jnp.add, [near[k] for k in range(16)])
    for k in range(1, 16):
        spread(far, k, far_ids, 1).start()
    grads_2.wait_recv()
    grads_3.start()
    wait_bytes(cand_g.at[pl.ds(0, 2)], pair_recv.at[2])
    lax.fori_loop(0, 16, choose_grads, 0)

    for part in range(3):
        for phase in range(3):
            sent = landing[part][phase] if phase < 2 else data[part][2].at[pl.ds(0, 3)]
            wait_bytes(sent, ring_send.at[part * 3 + phase])
    wait_bytes(cand, pair_send.at[0])
    wait_bytes(cand_g, pair_send.at[1])
    wait_bytes(near.at[pl.ds(1, 15)], norm_send.at[0])
    wait_bytes(far.at[pl.ds(1, 15)], norm_send.at[1])
    wait_bytes(far.at[pl.ds(1, 15)], norm_recv.at[1])
    squares_sum[...] = functools.reduce(jnp.add, [far[k] for k in range(16)])


def update_kernel(state, squares_sum, out_w, out_m, out_v, buf, sem):
    norm2 = jnp.sum(squares_sum[...], axis=1, keepdims=True)
    scale = 1.0 / jnp.maximum(jnp.sqrt(norm2 / (4 * N_DP * SH)), 1.0)
    outs = (out_w, out_m, out_v)
    n = SH // 4

    def copies(q):
        cols = pl.ds(pl.multiple_of(q * n, n), n)
        return [pltpu.make_async_copy(buf.at[a, :, cols], outs[a].at[0, 0, :, cols], sem.at[a]) for a in range(3)]

    def quarter(q, carry):
        for i in range(n // 512):
            cols = pl.ds(pl.multiple_of(q * n + i * 512, 512), 512)
            weights, first, second, total = [state[a, :, cols] for a in range(4)]
            scaled = scale * total
            first_new = beta_one * first + (1.0 - beta_one) * scaled
            second_new = beta_two * second + (1.0 - beta_two) * scaled * scaled
            change = first_new / bias_one / (jnp.sqrt(second_new / bias_two) + eps_value) + decay * weights
            buf[0, :, cols] = weights - rate * change
            buf[1, :, cols] = first_new
            buf[2, :, cols] = second_new
        for c in copies(q):
            c.start()
        return carry

    lax.fori_loop(0, 4, quarter, 0)
    for a in range(3):
        pltpu.make_async_copy(buf.at[a], outs[a].at[0, 0], sem.at[a]).wait()


def on_device(master, moment1, moment2, local_grad, partner):
    f32 = jnp.float32
    vmem = [pltpu.VMEM((4, 4, 4, p[2], 128), f32) for p in PARTS]
    vmem += [pltpu.VMEM((6, 2, 4, p[2], 128), f32) for p in PARTS]
    vmem += [pltpu.VMEM((4, 4, p[2], 128), f32) for p in PARTS]
    vmem += [pltpu.VMEM((6, 2, p[2], 128), f32) for p in PARTS]
    vmem += [pltpu.VMEM((4, p[2], 128), f32) for p in PARTS]
    vmem += [pltpu.VMEM((6, p[3], 128), f32) for p in PARTS]
    dma = pltpu.SemaphoreType.DMA
    out = jax.ShapeDtypeStruct((1, 1, 2, SH), f32)
    state, squares_sum = pl.pallas_call(
        kernel,
        out_shape=(pltpu.VMEM((4, 2, SH), f32), pltpu.VMEM((1, 128), f32)),
        in_specs=[pl.BlockSpec(memory_space=pltpu.SMEM)] + [pl.BlockSpec(memory_space=pltpu.HBM)] * 4,
        out_specs=[pl.BlockSpec(memory_space=pltpu.VMEM)] * 2,
        scratch_shapes=[
            pltpu.VMEM((1, N_DP * SH), jnp.bfloat16),
            pltpu.VMEM((3, 1, SH), f32),
            pltpu.VMEM((3, 3, 1, SH), f32),
            pltpu.VMEM((128, 128), f32),
            pltpu.VMEM((3, 128, 128), f32),
            pltpu.VMEM((16, 1, 128), f32),
            pltpu.VMEM((16, 1, 128), f32),
        ]
        + vmem
        + [dma((4,)), dma, dma((9,)), dma((27,)), dma((2,)), dma((4,)), dma((2,)), dma((2,))],
        compiler_params=pltpu.CompilerParams(collective_id=0, has_side_effects=True),
        name="step",
    )(partner, master, moment1, moment2, local_grad)
    return pl.pallas_call(
        update_kernel,
        out_shape=(out, out, out),
        in_specs=[pl.BlockSpec(memory_space=pltpu.VMEM)] * 2,
        out_specs=[pl.BlockSpec(memory_space=pltpu.HBM)] * 3,
        scratch_shapes=[pltpu.VMEM((3, 2, SH), f32), dma((3,))],
        name="update",
    )(*[pltpu.with_memory_space_constraint(v, pltpu.VMEM) for v in (state, squares_sum)])


def solution(mesh):
    finer = Mesh(mesh.devices.reshape(2, 2, 4, 4, 4), PAIR + DP)
    in_specs = (P(PAIR, DP), P(PAIR, DP), P(PAIR, DP), P(PAIR, DP, None), P(DP, None))
    out_specs = (P(PAIR, DP, None, None),) * 3
    return jax.shard_map(on_device, mesh=finer, in_specs=in_specs, out_specs=out_specs, check_vma=False)
```

```python
import functools

import jax
import jax.numpy as jnp
from jax import lax
from jax.experimental import pallas as pl
from jax.experimental.pallas import tpu as pltpu
from jax.sharding import Mesh
from jax.sharding import PartitionSpec as P

beta_one = 0.9
beta_two = 0.95
bias_one = 1.0 - 0.9**10
bias_two = 1.0 - 0.95**10
rate = 0.001
decay = 0.1
eps_value = 1e-08

SH = 16384
N_DP = 64
PAIR = ("zl", "core")
DP = ("zh", "x", "y")
STRIDE = {"zh": 16, "x": 4, "y": 1}
MESH = pl.DeviceIdType.MESH

PARTS = (
    (("x", "y", "zh"), 0, 56, 32),
    (("y", "x", "zh"), 56, 56, 32),
    (("zh", "x", "y"), 112, 16, 8),
)
FIRST = (2, 0, 1)
AP, AM, BP, BM, CP, CM = range(6)


def kernel(
    partner, w_hbm, m_hbm, v_hbm, g_hbm, state, squares_sum,
    stage, own, cand, grads, cand_g, near, far,
    f0, f1, f2, r0, r1, r2, s0, s1, s2, q0, q1, q2, t0, t1, t2, u0, u1, u2,
    load_sem, own_sem, ring_send, ring_recv, pair_send, pair_recv, norm_send, norm_recv,
):
    data = ((f0, s0, t0), (f1, s1, t1), (f2, s2, t2))
    landing = ((r0, q0, u0), (r1, q1, u1), (r2, q2, u2))
    at = {a: lax.axis_index(a) for a in PAIR + DP}

    def beside(axis, step):
        return lax.rem(at[axis] + step + 4, 4)

    groups = (2, 1, -1, 0)
    for i in groups:
        for zh in range(4):
            cols = pl.ds((zh * 16 + beside("x", i) * 4) * SH, 4 * SH)
            pltpu.make_async_copy(g_hbm.at[0, :, cols], stage.at[:, cols], load_sem.at[i % 4]).start()
    for i, ref in enumerate((w_hbm, m_hbm, v_hbm)):
        pltpu.make_async_copy(ref, own.at[i], own_sem).start()

    def loaded(i):
        part_of = stage.at[:, pl.ds(0, 16 * SH)]
        pltpu.make_async_copy(part_of, part_of, load_sem.at[i % 4]).wait()

    barrier = pltpu.get_barrier_semaphore()
    near_ids = [
        {"zh": beside("zh", k // 4), "zl": lax.rem(at["zl"] + (k // 2) % 2, 2), "core": lax.rem(at["core"] + k % 2, 2)}
        for k in range(16)
    ]
    far_ids = [{"x": beside("x", k // 4), "y": beside("y", k % 4)} for k in range(16)]
    for axis in DP:
        for step in (1, -1):
            pl.semaphore_signal(barrier, inc=1, device_id={axis: beside(axis, step)}, device_id_type=MESH)
    for axis in PAIR:
        pl.semaphore_signal(barrier, inc=1, device_id={axis: 1 - at[axis]}, device_id_type=MESH)

    def convert(part, c0, half):
        order, row, rows, _ = PARTS[part]
        dst = data[part][0]

        def body(i, carry):
            c1 = half * 2 + i // 4
            c2 = lax.rem(i, 4)
            block = c0 * STRIDE[order[0]] + c1 * STRIDE[order[1]] + c2 * STRIDE[order[2]]
            for j in range(rows // 8):
                piece = stage[0:1, pl.ds(pl.multiple_of(block * SH + (row + 8 * j) * 128, 1024), 1024)]
                dst[c0, c1, c2, pl.ds(8 * j, 8), :] = piece.astype(jnp.float32).reshape(8, 128)
            return carry

        lax.fori_loop(0, 8, body, 0)

    def view(part, phase, c, half):
        ref = data[part][phase]
        if phase < 2:
            return ref.at[c, pl.ds(2 * half, 2)]
        cut, rows = PARTS[part][3], PARTS[part][2]
        return ref.at[c, pl.ds(0, cut)] if half == 0 else ref.at[c, pl.ds(cut, rows - cut)]

    def landed(part, phase, kind, half):
        ref = landing[part][phase].at[kind]
        if phase < 2:
            return ref
        cut, rows = PARTS[part][3], PARTS[part][2]
        return ref.at[pl.ds(0, cut if half == 0 else rows - cut)]

    HALF = {AP: 0, AM: 1, BP: 1, BM: 0, CP: 0, CM: 1}
    CHUNK = {AP: 2, AM: -2, BP: 1, BM: -1, CP: 1, CM: -1}

    def ring(part, phase, kind):
        axis = PARTS[part][0][phase]
        n = part * 3 + phase
        return pltpu.make_async_remote_copy(
            src_ref=view(part, phase, beside(axis, CHUNK[kind]), HALF[kind]),
            dst_ref=landed(part, phase, kind, HALF[kind]),
            send_sem=ring_send.at[n],
            recv_sem=ring_recv.at[n * 3 + min(kind, BP)],
            device_id={axis: beside(axis, 1 if kind in (AP, BP, CP) else -1)},
            device_id_type=MESH,
        )

    def wait_bytes(ref, sem):
        pltpu.make_async_copy(ref, ref, sem).wait()

    def flat(ref):
        shape = ref.shape
        rows = shape[-2] // 8
        lead = [()]
        for n in shape[:-2]:
            lead = [i + (j,) for i in lead for j in range(n)]
        return lead, rows

    def add_up(dst, *srcs):
        lead, rows = flat(dst)
        if len(lead) > 2:
            n1 = dst.shape[1]

            def body(i, carry):
                idx = (i // n1, lax.rem(i, n1))
                for j in range(rows):
                    tile = idx + (pl.ds(8 * j, 8), slice(None))
                    total = srcs[0][tile]
                    for s in srcs[1:]:
                        total = total + s[tile]
                    dst[tile] = total
                return carry

            lax.fori_loop(0, len(lead), body, 0)
        else:
            for idx in lead:
                for j in range(rows):
                    tile = idx + (pl.ds(8 * j, 8), slice(None))
                    total = srcs[0][tile]
                    for s in srcs[1:]:
                        total = total + s[tile]
                    dst[tile] = total

    def open_phase(part, phase):
        for kind in (AP, AM, BP, BM):
            ring(part, phase, kind).start()

    def forward(part, phase):
        axis = PARTS[part][0][phase]
        for a, c in ((AP, CP), (AM, CM)):
            ring(part, phase, a).wait_recv()
            mine = view(part, phase, beside(axis, CHUNK[c]), HALF[c])
            add_up(mine, mine, landed(part, phase, a, HALF[a]))
            ring(part, phase, c).start()

    def close_phase(part, phase):
        axis = PARTS[part][0][phase]
        last = data[part][2].at[pl.ds(0, 2)]
        wait_bytes(last if phase == 2 else landing[part][phase].at[pl.ds(2, 4)], ring_recv.at[(part * 3 + phase) * 3 + BP])
        for half, b, c in ((0, BM, CP), (1, BP, CM)):
            srcs = (
                view(part, phase, at[axis], half),
                landed(part, phase, b, half),
                landed(part, phase, c, half),
            )
            if phase < 2:
                add_up(data[part][phase + 1].at[pl.ds(2 * half, 2)], *srcs)
            else:
                row, rows, cut = PARTS[part][1:]
                lo, n = (0, cut) if half == 0 else (cut, rows - cut)
                add_up(grads.at[pl.ds(row + lo, n)], *srcs)

    for part in (0, 1, 2):
        axis = PARTS[part][0][0]
        for i in groups[:1] if part == 0 else groups[1:] if part == 1 else ():
            loaded(i)
        convert(part, beside(axis, 2), 0)
        convert(part, beside(axis, 2), 1)
        if part == 0:
            pl.semaphore_wait(barrier, 8)
        ring(part, 0, AP).start()
        ring(part, 0, AM).start()
    for part in (0, 1, 2):
        axis = PARTS[part][0][0]
        convert(part, beside(axis, 1), 1)
        convert(part, beside(axis, -1), 0)
        ring(part, 0, BP).start()
        ring(part, 0, BM).start()
    for part in FIRST:
        axis = PARTS[part][0][0]
        convert(part, beside(axis, 1), 0)
        convert(part, beside(axis, -1), 1)
        convert(part, at[axis], 0)
        convert(part, at[axis], 1)
    for part in FIRST:
        forward(part, 0)

    def pair_copy(src, dst, n, axis):
        return pltpu.make_async_remote_copy(
            src_ref=src, dst_ref=dst, send_sem=pair_send.at[n // 2], recv_sem=pair_recv.at[n],
            device_id={axis: 1 - at[axis]}, device_id_type=MESH,
        )

    wait_bytes(own, own_sem)
    shard_1 = pair_copy(own, cand.at[0], 0, "core")
    shard_2 = pair_copy(own, cand.at[2], 1, "zl")
    shard_3 = pair_copy(cand.at[2], cand.at[1], 0, "core")

    mine = at["zl"] * 2 + at["core"]
    mate = partner[0, mine]
    apart = jnp.full((1, 1024), mine ^ mate, jnp.int32)
    is_one, is_two = apart == 1, apart == 2
    survive = jnp.full((1, 1024), mate - mine, jnp.int32) > 0

    def keep(a, cols, value, values):
        theirs = jnp.where(is_one, values[0], jnp.where(is_two, values[1], values[2]))
        state[a, 0:1, cols] = jnp.where(survive, value, 0.0)
        state[a, 1:2, cols] = jnp.where(survive, theirs, 0.0)

    def choose(i, carry):
        cols = pl.ds(pl.multiple_of(i * 1024, 1024), 1024)
        for a in range(3):
            keep(a, cols, own[a, :, cols], [cand[k, a, :, cols] for k in (0, 2, 1)])
        return carry

    def choose_grads(i, carry):
        cols = pl.ds(pl.multiple_of(i * 1024, 1024), 1024)
        rows = pl.ds(pl.multiple_of(i * 8, 8), 8)
        keep(3, cols, grads[rows, :].reshape(1, 1024), [cand_g[k, rows, :].reshape(1, 1024) for k in (0, 2, 1)])
        return carry

    for phase in (0, 1, 2):
        for part in FIRST:
            close_phase(part, phase)
            if phase < 2:
                open_phase(part, phase + 1)
            if phase == 0 and part == FIRST[0]:
                shard_1.start()
                shard_2.start()
        if phase < 2:
            for part in FIRST:
                forward(part, phase + 1)
        if phase == 0:
            shard_2.wait_recv()
            shard_3.start()
        if phase == 1:
            wait_bytes(cand.at[pl.ds(0, 2)], pair_recv.at[0])
            lax.fori_loop(0, 16, choose, 0)

    def squares(i, total):
        tile = grads[pl.ds(pl.multiple_of(i * 8, 8), 8), :]
        return total + tile * tile

    total = lax.fori_loop(0, 16, squares, jnp.zeros((8, 128), jnp.float32))
    near[0] = jnp.sum(total, axis=0, keepdims=True)

    def spread(buf, k, ids, n):
        return pltpu.make_async_remote_copy(
            src_ref=buf.at[0], dst_ref=buf.at[k], send_sem=norm_send.at[n], recv_sem=norm_recv.at[n],
            device_id=ids[k], device_id_type=MESH,
        )

    grads_1 = pair_copy(grads, cand_g.at[0], 2, "core")
    grads_2 = pair_copy(grads, cand_g.at[2], 3, "zl")
    grads_3 = pair_copy(cand_g.at[2], cand_g.at[1], 2, "core")
    for k in range(1, 16):
        spread(near, k, near_ids, 0).start()
    grads_1.start()
    grads_2.start()
    wait_bytes(near.at[pl.ds(1, 15)], norm_recv.at[0])
    far[0] = functools.reduce(jnp.add, [near[k] for k in range(16)])
    for k in range(1, 16):
        spread(far, k, far_ids, 1).start()
    grads_2.wait_recv()
    grads_3.start()
    wait_bytes(cand_g.at[pl.ds(0, 2)], pair_recv.at[2])
    lax.fori_loop(0, 16, choose_grads, 0)

    for part in range(3):
        for phase in range(3):
            sent = landing[part][phase] if phase < 2 else data[part][2].at[pl.ds(0, 3)]
            wait_bytes(sent, ring_send.at[part * 3 + phase])
    wait_bytes(cand, pair_send.at[0])
    wait_bytes(cand_g, pair_send.at[1])
    wait_bytes(near.at[pl.ds(1, 15)], norm_send.at[0])
    wait_bytes(far.at[pl.ds(1, 15)], norm_send.at[1])
    wait_bytes(far.at[pl.ds(1, 15)], norm_recv.at[1])
    squares_sum[...] = functools.reduce(jnp.add, [far[k] for k in range(16)])


def update_kernel(state, squares_sum, out_w, out_m, out_v, buf, sem):
    norm2 = jnp.sum(squares_sum[...], axis=1, keepdims=True)
    scale = 1.0 / jnp.maximum(jnp.sqrt(norm2 / (4 * N_DP * SH)), 1.0)
    outs = (out_w, out_m, out_v)
    n = SH // 4

    def copies(q):
        cols = pl.ds(pl.multiple_of(q * n, n), n)
        return [pltpu.make_async_copy(buf.at[a, :, cols], outs[a].at[0, 0, :, cols], sem.at[a]) for a in range(3)]

    def quarter(q, carry):
        for i in range(n // 512):
            cols = pl.ds(pl.multiple_of(q * n + i * 512, 512), 512)
            weights, first, second, total = [state[a, :, cols] for a in range(4)]
            scaled = scale * total
            first_new = beta_one * first + (1.0 - beta_one) * scaled
            second_new = beta_two * second + (1.0 - beta_two) * scaled * scaled
            change = first_new / bias_one / (jnp.sqrt(second_new / bias_two) + eps_value) + decay * weights
            buf[0, :, cols] = weights - rate * change
            buf[1, :, cols] = first_new
            buf[2, :, cols] = second_new
        for c in copies(q):
            c.start()
        return carry

    lax.fori_loop(0, 4, quarter, 0)
    for a in range(3):
        pltpu.make_async_copy(buf.at[a], outs[a].at[0, 0], sem.at[a]).wait()


def on_device(master, moment1, moment2, local_grad, partner):
    f32 = jnp.float32
    vmem = [pltpu.VMEM((4, 4, 4, p[2], 128), f32) for p in PARTS]
    vmem += [pltpu.VMEM((6, 2, 4, p[2], 128), f32) for p in PARTS]
    vmem += [pltpu.VMEM((4, 4, p[2], 128), f32) for p in PARTS]
    vmem += [pltpu.VMEM((6, 2, p[2], 128), f32) for p in PARTS]
    vmem += [pltpu.VMEM((4, p[2], 128), f32) for p in PARTS]
    vmem += [pltpu.VMEM((6, p[3], 128), f32) for p in PARTS]
    dma = pltpu.SemaphoreType.DMA
    out = jax.ShapeDtypeStruct((1, 1, 2, SH), f32)
    state, squares_sum = pl.pallas_call(
        kernel,
        out_shape=(pltpu.VMEM((4, 2, SH), f32), pltpu.VMEM((1, 128), f32)),
        in_specs=[pl.BlockSpec(memory_space=pltpu.SMEM)] + [pl.BlockSpec(memory_space=pltpu.HBM)] * 4,
        out_specs=[pl.BlockSpec(memory_space=pltpu.VMEM)] * 2,
        scratch_shapes=[
            pltpu.VMEM((1, N_DP * SH), jnp.bfloat16),
            pltpu.VMEM((3, 1, SH), f32),
            pltpu.VMEM((3, 3, 1, SH), f32),
            pltpu.VMEM((128, 128), f32),
            pltpu.VMEM((3, 128, 128), f32),
            pltpu.VMEM((16, 1, 128), f32),
            pltpu.VMEM((16, 1, 128), f32),
        ]
        + vmem
        + [dma((4,)), dma, dma((9,)), dma((27,)), dma((2,)), dma((4,)), dma((2,)), dma((2,))],
        compiler_params=pltpu.CompilerParams(collective_id=0, has_side_effects=True),
        name="step",
    )(partner, master, moment1, moment2, local_grad)
    return pl.pallas_call(
        update_kernel,
        out_shape=(out, out, out),
        in_specs=[pl.BlockSpec(memory_space=pltpu.VMEM)] * 2,
        out_specs=[pl.BlockSpec(memory_space=pltpu.HBM)] * 3,
        scratch_shapes=[pltpu.VMEM((3, 2, SH), f32), dma((3,))],
        name="update",
    )(*[pltpu.with_memory_space_constraint(v, pltpu.VMEM) for v in (state, squares_sum)])


def solution(mesh):
    finer = Mesh(mesh.devices.reshape(2, 2, 4, 4, 4), PAIR + DP)
    in_specs = (P(PAIR, DP), P(PAIR, DP), P(PAIR, DP), P(PAIR, DP, None), P(DP, None))
    out_specs = (P(PAIR, DP, None, None),) * 3
    return jax.shard_map(on_device, mesh=finer, in_specs=in_specs, out_specs=out_specs, check_vma=False)
```

```python
import functools

import jax
import jax.numpy as jnp
from jax import lax
from jax.experimental import pallas as pl
from jax.experimental.pallas import tpu as pltpu
from jax.sharding import Mesh
from jax.sharding import PartitionSpec as P

beta_one = 0.9
beta_two = 0.95
bias_one = 1.0 - 0.9**10
bias_two = 1.0 - 0.95**10
rate = 0.001
decay = 0.1
eps_value = 1e-08

SH = 16384
N_DP = 64
PAIR = ("zl", "core")
DP = ("zh", "x", "y")
STRIDE = {"zh": 16, "x": 4, "y": 1}
MESH = pl.DeviceIdType.MESH

XYZ, YXZ, ZXY, ZYX = ("x", "y", "zh"), ("y", "x", "zh"), ("zh", "x", "y"), ("zh", "y", "x")
PARTS = (
    (ZXY, 12, 8),
    (ZYX, 12, 8),
    (XYZ, 32, 16),
    (YXZ, 32, 16),
    (XYZ, 20, 12),
    (YXZ, 20, 12),
)
START = tuple(sum(p[1] for p in PARTS[:i]) for i in range(len(PARTS)))
EARLY = 4
LOADING = (2, 3, 0, 1) + tuple(range(4, len(PARTS)))
ORDER_A = (2,3,4,5,0,1)
ORDER_SUM = (2,3,0,1,4,5)
ORDER_LATER = (0,1,2,3,4,5)
AP, AM, BP, BM, CP, CM = range(6)


def kernel(
    partner, w_hbm, m_hbm, v_hbm, g_hbm, state, squares_sum,
    stage, own, cand, grads, cand_g, near, far,
    load_sem, own_sem, ring_send, ring_recv, pair_send, pair_recv, norm_send, norm_recv, *ring_bufs,
):
    data = [ring_bufs[6 * p : 6 * p + 3] for p in range(len(PARTS))]
    landing = [ring_bufs[6 * p + 3 : 6 * p + 6] for p in range(len(PARTS))]
    at = {a: lax.axis_index(a) for a in PAIR + DP}

    def beside(axis, step):
        return lax.rem(at[axis] + step + 4, 4)

    groups = (2, 1, -1, 0)
    for i in groups:
        for zh in range(4):
            cols = pl.ds((zh * 16 + beside("x", i) * 4) * SH, 4 * SH)
            pltpu.make_async_copy(g_hbm.at[0, :, cols], stage.at[:, cols], load_sem.at[i % 4]).start()
    for i, ref in enumerate((w_hbm, m_hbm, v_hbm)):
        pltpu.make_async_copy(ref, own.at[i], own_sem).start()

    def loaded(i):
        part_of = stage.at[:, pl.ds(0, 16 * SH)]
        pltpu.make_async_copy(part_of, part_of, load_sem.at[i % 4]).wait()

    barrier = pltpu.get_barrier_semaphore()
    near_ids = [
        {"zh": beside("zh", k // 4), "zl": lax.rem(at["zl"] + (k // 2) % 2, 2), "core": lax.rem(at["core"] + k % 2, 2)}
        for k in range(16)
    ]
    far_ids = [{"x": beside("x", k // 4), "y": beside("y", k % 4)} for k in range(16)]
    for axis in DP:
        for step in (1, -1):
            pl.semaphore_signal(barrier, inc=1, device_id={axis: beside(axis, step)}, device_id_type=MESH)
    for axis in PAIR:
        pl.semaphore_signal(barrier, inc=1, device_id={axis: 1 - at[axis]}, device_id_type=MESH)

    def pieces(width):
        return [pl.ds(lo, min(1024, width - lo)) for lo in range(0, width, 1024)]

    def convert(part, c0, half):
        order, rows, _ = PARTS[part]
        dst = data[part][0]
        for c1 in (2 * half, 2 * half + 1):

            def body(c2, carry, c1=c1):
                block = c0 * STRIDE[order[0]] + c1 * STRIDE[order[1]] + c2 * STRIDE[order[2]]
                for p in pieces(rows * 128):
                    cols = pl.ds(pl.multiple_of(block * SH + START[part] * 128 + p.start, 128), p.size)
                    dst[c0, c1, c2, :, p] = stage[0:1, cols].astype(jnp.float32)
                return carry

            lax.fori_loop(0, 4, body, 0)

    def halves(part):
        rows, cut = PARTS[part][1:]
        return pl.ds(0, cut * 128), pl.ds(cut * 128, (rows - cut) * 128)

    def view(part, phase, c, half):
        ref = data[part][phase]
        return ref.at[c, pl.ds(2 * half, 2)] if phase < 2 else ref.at[c, :, halves(part)[half]]

    def landed(part, phase, kind, half):
        ref = landing[part][phase].at[kind]
        return ref if phase < 2 else ref.at[:, pl.ds(0, halves(part)[half].size)]

    HALF = {AP: 0, AM: 1, BP: 1, BM: 0, CP: 0, CM: 1}
    CHUNK = {AP: 2, AM: -2, BP: 1, BM: -1, CP: 1, CM: -1}

    def ring(part, phase, kind):
        axis = PARTS[part][0][phase]
        n = part * 3 + phase
        return pltpu.make_async_remote_copy(
            src_ref=view(part, phase, beside(axis, CHUNK[kind]), HALF[kind]),
            dst_ref=landed(part, phase, kind, HALF[kind]),
            send_sem=ring_send.at[n],
            recv_sem=ring_recv.at[n * 3 + min(kind, BP)],
            device_id={axis: beside(axis, 1 if kind in (AP, BP, CP) else -1)},
            device_id_type=MESH,
        )

    def wait_bytes(ref, sem):
        pltpu.make_async_copy(ref, ref, sem).wait()

    def add_up(dst, *srcs):
        lead, width = dst.shape[:-2], dst.shape[-1]

        def one(idx):
            for p in pieces(width):
                at_p = idx + (slice(None), p)
                total = srcs[0][at_p]
                for s in srcs[1:]:
                    total = total + s[at_p]
                dst[at_p] = total

        if len(lead) == 2:

            def body(i, carry):
                for j in range(lead[0]):
                    one((j, i))
                return carry

            lax.fori_loop(0, lead[1], body, 0)
        else:
            for j in range(lead[0] if lead else 1):
                one((j,) if lead else ())

    def open_phase(part, phase):
        for kind in (AP, AM, BP, BM):
            ring(part, phase, kind).start()

    def forward(part, phase):
        axis = PARTS[part][0][phase]
        for a, c in ((AP, CP), (AM, CM)):
            ring(part, phase, a).wait_recv()
            mine = view(part, phase, beside(axis, CHUNK[c]), HALF[c])
            add_up(mine, mine, landed(part, phase, a, HALF[a]))
            ring(part, phase, c).start()

    def close_phase(part, phase):
        axis = PARTS[part][0][phase]
        last = data[part][2].at[pl.ds(0, 2)]
        wait_bytes(last if phase == 2 else landing[part][phase].at[pl.ds(2, 4)], ring_recv.at[(part * 3 + phase) * 3 + BP])
        for half, b, c in ((0, BM, CP), (1, BP, CM)):
            srcs = (
                view(part, phase, at[axis], half),
                landed(part, phase, b, half),
                landed(part, phase, c, half),
            )
            if phase < 2:
                add_up(data[part][phase + 1].at[pl.ds(2 * half, 2)], *srcs)
            else:
                cols = halves(part)[half]
                add_up(grads.at[:, pl.ds(START[part] * 128 + cols.start, cols.size)], *srcs)

    for n, part in enumerate(LOADING):
        axis = PARTS[part][0][0]
        for i in (groups[:1], groups[1:])[n] if n < 2 else ():
            loaded(i)
        convert(part, beside(axis, 2), 0)
        convert(part, beside(axis, 2), 1)
        if n == 0:
            pl.semaphore_wait(barrier, 8)
        ring(part, 0, AP).start()
        ring(part, 0, AM).start()
    for part in LOADING:
        axis = PARTS[part][0][0]
        convert(part, beside(axis, 1), 1)
        convert(part, beside(axis, -1), 0)
        ring(part, 0, BP).start()
        ring(part, 0, BM).start()
    for part in LOADING:
        axis = PARTS[part][0][0]
        convert(part, beside(axis, 1), 0)
        convert(part, beside(axis, -1), 1)
    for part in ORDER_A:
        forward(part, 0)
    for part in LOADING:
        axis = PARTS[part][0][0]
        convert(part, at[axis], 0)
        convert(part, at[axis], 1)

    def pair_copy(src, dst, n, axis):
        return pltpu.make_async_remote_copy(
            src_ref=src, dst_ref=dst, send_sem=pair_send.at[n // 2], recv_sem=pair_recv.at[n],
            device_id={axis: 1 - at[axis]}, device_id_type=MESH,
        )

    wait_bytes(own, own_sem)
    shard_1 = pair_copy(own, cand.at[0], 0, "core")
    shard_2 = pair_copy(own, cand.at[2], 1, "zl")
    shard_3 = pair_copy(cand.at[2], cand.at[1], 0, "core")

    mine = at["zl"] * 2 + at["core"]
    mate = partner[0, mine]
    apart = jnp.full((1, 1024), mine ^ mate, jnp.int32)
    is_one, is_two = apart == 1, apart == 2
    survive = jnp.full((1, 1024), mate - mine, jnp.int32) > 0

    def keep(a, cols, value, values):
        theirs = jnp.where(is_one, values[0], jnp.where(is_two, values[1], values[2]))
        state[a, 0:1, cols] = jnp.where(survive, value, 0.0)
        state[a, 1:2, cols] = jnp.where(survive, theirs, 0.0)

    def choose(i, carry):
        cols = pl.ds(pl.multiple_of(i * 1024, 1024), 1024)
        for a in range(3):
            keep(a, cols, own[a, :, cols], [cand[k, a, :, cols] for k in (0, 2, 1)])
        return carry

    def choose_grads(i, carry):
        cols = pl.ds(pl.multiple_of(i * 1024, 1024), 1024)
        keep(3, cols, grads[:, cols], [cand_g[k, :, cols] for k in (0, 2, 1)])
        return carry

    early = START[EARLY] * 128
    shares = (pl.ds(0, early), pl.ds(early, SH - early))

    def grads_copy(step, share):
        src = cand_g.at[2] if step == 2 else grads
        return pair_copy(
            src.at[:, shares[share]], cand_g.at[(0, 2, 1)[step], :, shares[share]], 2 + 2 * share + step % 2, ("core", "zl", "core")[step]
        )

    for phase in (0, 1, 2):
        for part in ORDER_LATER if phase else ORDER_SUM:
            close_phase(part, phase)
            if phase < 2:
                open_phase(part, phase + 1)
            elif part == EARLY - 1:
                grads_copy(0, 0).start()
                grads_copy(1, 0).start()
            if phase == 0 and part == 1:
                shard_1.start()
                shard_2.start()
        if phase < 2:
            for part in ORDER_LATER:
                forward(part, phase + 1)
        if phase == 0:
            shard_2.wait_recv()
            shard_3.start()
        if phase == 1:
            wait_bytes(cand.at[pl.ds(0, 2)], pair_recv.at[0])
            lax.fori_loop(0, 16, choose, 0)

    def squares(i, total):
        tile = grads[:, pl.ds(pl.multiple_of(i * 1024, 1024), 1024)]
        return total + tile * tile

    total = lax.fori_loop(0, 16, squares, jnp.zeros((1, 1024), jnp.float32))
    near[0] = jnp.sum(total.reshape(8, 128), axis=0, keepdims=True)

    def spread(buf, k, ids, n):
        return pltpu.make_async_remote_copy(
            src_ref=buf.at[0], dst_ref=buf.at[k], send_sem=norm_send.at[n], recv_sem=norm_recv.at[n],
            device_id=ids[k], device_id_type=MESH,
        )

    for k in range(1, 16):
        spread(near, k, near_ids, 0).start()
    grads_copy(0, 1).start()
    grads_copy(1, 1).start()
    grads_copy(1, 0).wait_recv()
    grads_copy(2, 0).start()
    wait_bytes(near.at[pl.ds(1, 15)], norm_recv.at[0])
    far[0] = functools.reduce(jnp.add, [near[k] for k in range(16)])
    for k in range(1, 16):
        spread(far, k, far_ids, 1).start()
    grads_copy(1, 1).wait_recv()
    grads_copy(2, 1).start()
    for share in (0, 1):
        wait_bytes(cand_g.at[pl.ds(0, 2), :, shares[share]], pair_recv.at[2 + 2 * share])
    lax.fori_loop(0, 16, choose_grads, 0)

    for part in range(len(PARTS)):
        for phase in range(3):
            sent = landing[part][phase] if phase < 2 else data[part][2].at[pl.ds(0, 3)]
            wait_bytes(sent, ring_send.at[part * 3 + phase])
    wait_bytes(cand, pair_send.at[0])
    for share in (0, 1):
        wait_bytes(cand_g.at[:, :, shares[share]], pair_send.at[1 + share])
    wait_bytes(near.at[pl.ds(1, 15)], norm_send.at[0])
    wait_bytes(far.at[pl.ds(1, 15)], norm_send.at[1])
    wait_bytes(far.at[pl.ds(1, 15)], norm_recv.at[1])
    squares_sum[...] = functools.reduce(jnp.add, [far[k] for k in range(16)])


def update_kernel(state, squares_sum, out_w, out_m, out_v, buf, sem):
    norm2 = jnp.sum(squares_sum[...], axis=1, keepdims=True)
    scale = 1.0 / jnp.maximum(jnp.sqrt(norm2 / (4 * N_DP * SH)), 1.0)
    outs = (out_w, out_m, out_v)
    n = SH // 4

    def copies(q):
        cols = pl.ds(pl.multiple_of(q * n, n), n)
        return [pltpu.make_async_copy(buf.at[a, :, cols], outs[a].at[0, 0, :, cols], sem.at[a]) for a in range(3)]

    def quarter(q, carry):
        for i in range(n // 512):
            cols = pl.ds(pl.multiple_of(q * n + i * 512, 512), 512)
            weights, first, second, total = [state[a, :, cols] for a in range(4)]
            scaled = scale * total
            first_new = beta_one * first + (1.0 - beta_one) * scaled
            second_new = beta_two * second + (1.0 - beta_two) * scaled * scaled
            change = first_new / bias_one / (jnp.sqrt(second_new / bias_two) + eps_value) + decay * weights
            buf[0, :, cols] = weights - rate * change
            buf[1, :, cols] = first_new
            buf[2, :, cols] = second_new
        for c in copies(q):
            c.start()
        return carry

    lax.fori_loop(0, 4, quarter, 0)
    for a in range(3):
        pltpu.make_async_copy(buf.at[a], outs[a].at[0, 0], sem.at[a]).wait()


def on_device(master, moment1, moment2, local_grad, partner):
    f32 = jnp.float32
    vmem = []
    for _, rows, cut in PARTS:
        vmem += [pltpu.VMEM(n + (1, rows * 128), f32) for n in ((4, 4, 4), (4, 4), (4,), (6, 2, 4), (6, 2))]
        vmem.append(pltpu.VMEM((6, 1, max(cut, rows - cut) * 128), f32))
    dma = pltpu.SemaphoreType.DMA
    out = jax.ShapeDtypeStruct((1, 1, 2, SH), f32)
    state, squares_sum = pl.pallas_call(
        kernel,
        out_shape=(pltpu.VMEM((4, 2, SH), f32), pltpu.VMEM((1, 128), f32)),
        in_specs=[pl.BlockSpec(memory_space=pltpu.SMEM)] + [pl.BlockSpec(memory_space=pltpu.HBM)] * 4,
        out_specs=[pl.BlockSpec(memory_space=pltpu.VMEM)] * 2,
        scratch_shapes=[
            pltpu.VMEM((1, N_DP * SH), jnp.bfloat16),
            pltpu.VMEM((3, 1, SH), f32),
            pltpu.VMEM((3, 3, 1, SH), f32),
            pltpu.VMEM((1, SH), f32),
            pltpu.VMEM((3, 1, SH), f32),
            pltpu.VMEM((16, 1, 128), f32),
            pltpu.VMEM((16, 1, 128), f32),
        ]
        + [dma((4,)), dma, dma((3 * len(PARTS),)), dma((9 * len(PARTS),)), dma((3,)), dma((6,)), dma((2,)), dma((2,))]
        + vmem,
        compiler_params=pltpu.CompilerParams(collective_id=0, has_side_effects=True),
        name="step",
    )(partner, master, moment1, moment2, local_grad)
    return pl.pallas_call(
        update_kernel,
        out_shape=(out, out, out),
        in_specs=[pl.BlockSpec(memory_space=pltpu.VMEM)] * 2,
        out_specs=[pl.BlockSpec(memory_space=pltpu.HBM)] * 3,
        scratch_shapes=[pltpu.VMEM((3, 2, SH), f32), dma((3,))],
        name="update",
    )(*[pltpu.with_memory_space_constraint(v, pltpu.VMEM) for v in (state, squares_sum)])


def solution(mesh):
    finer = Mesh(mesh.devices.reshape(2, 2, 4, 4, 4), PAIR + DP)
    in_specs = (P(PAIR, DP), P(PAIR, DP), P(PAIR, DP), P(PAIR, DP, None), P(DP, None))
    out_specs = (P(PAIR, DP, None, None),) * 3
    return jax.shard_map(on_device, mesh=finer, in_specs=in_specs, out_specs=out_specs, check_vma=False)
```

```python
import functools

import jax
import jax.numpy as jnp
from jax import lax
from jax.experimental import pallas as pl
from jax.experimental.pallas import tpu as pltpu
from jax.sharding import Mesh
from jax.sharding import PartitionSpec as P

beta_one = 0.9
beta_two = 0.95
bias_one = 1.0 - 0.9**10
bias_two = 1.0 - 0.95**10
rate = 0.001
decay = 0.1
eps_value = 1e-08

SH = 16384
N_DP = 64
PAIR = ("zl", "core")
DP = ("zh", "x", "y")
STRIDE = {"zh": 16, "x": 4, "y": 1}
MESH = pl.DeviceIdType.MESH

XYZ, YXZ, ZXY, ZYX = ("x", "y", "zh"), ("y", "x", "zh"), ("zh", "x", "y"), ("zh", "y", "x")
PARTS = (
    (ZXY, 12, 8, False),
    (ZYX, 12, 8, False),
    (XYZ, 24, 12, False),
    (YXZ, 24, 12, False),
    (XYZ, 16, 8, False),
    (YXZ, 16, 8, False),
    (XYZ, 12, 8, True),
    (YXZ, 12, 8, True),
)
START = tuple(sum(p[1] for p in PARTS[:i]) for i in range(len(PARTS)))
EARLY = 6
LOADING = (2, 3, 0, 1) + tuple(range(4, len(PARTS)))
ORDER_A = (2,3,4,5,0,1,6,7)
ORDER_SUM = (2,3,0,1,4,5,6,7)
ORDER_LATER = (2,3,0,1,4,5,6,7)
AP, AM, BP, BM, CP, CM = range(6)
RECV = [(i, phase, a) for i, p in enumerate(PARTS) for phase in range(3) for a in (True, False) if not (a and p[3] and phase)]
RECV = {key: n for n, key in enumerate(RECV)}


def kernel(
    partner_hbm, w_hbm, m_hbm, v_hbm, g_hbm, state, squares_sum,
    stage, own, cand, grads, cand_g, near, far,
    gauge, partner, partner_sem, load_sem, own_sem, ring_send, ring_recv, rest_send, pair_recv, norm_recv, *ring_bufs,
):
    data = [ring_bufs[6 * p : 6 * p + 3] for p in range(len(PARTS))]
    landing = [ring_bufs[6 * p + 3 : 6 * p + 6] for p in range(len(PARTS))]
    at = {a: lax.axis_index(a) for a in PAIR + DP}

    def beside(axis, step):
        return lax.rem(at[axis] + step + 4, 4)

    groups = (2, 1, -1, 0)
    for i in groups:
        for zh in range(4):
            cols = pl.ds((zh * 16 + beside("x", i) * 4) * SH, 4 * SH)
            pltpu.make_async_copy(g_hbm.at[0, :, cols], stage.at[:, cols], load_sem.at[i % 4]).start()
    for i, ref in enumerate((w_hbm, m_hbm, v_hbm)):
        pltpu.make_async_copy(ref, own.at[i], own_sem).start()

    partner_copy = pltpu.make_async_copy(partner_hbm, partner, partner_sem)
    partner_copy.start()

    def loaded(i):
        part_of = stage.at[:, pl.ds(0, 16 * SH)]
        pltpu.make_async_copy(part_of, part_of, load_sem.at[i % 4]).wait()

    barrier = pltpu.get_barrier_semaphore()
    near_ids = [
        {"zh": beside("zh", k // 4), "zl": lax.rem(at["zl"] + (k // 2) % 2, 2), "core": lax.rem(at["core"] + k % 2, 2)}
        for k in range(16)
    ]
    far_ids = [{"x": beside("x", k // 4), "y": beside("y", k % 4)} for k in range(16)]
    for axis in DP:
        for step in (1, -1):
            pl.semaphore_signal(barrier, inc=1, device_id={axis: beside(axis, step)}, device_id_type=MESH)
    for axis in PAIR:
        pl.semaphore_signal(barrier, inc=1, device_id={axis: 1 - at[axis]}, device_id_type=MESH)

    def pieces(width):
        return [pl.ds(lo, min(1024, width - lo)) for lo in range(0, width, 1024)]

    def convert(part, c0, half):
        order, rows = PARTS[part][:2]
        dst = data[part][0]
        for c1 in (2 * half, 2 * half + 1):

            def body(c2, carry, c1=c1):
                block = c0 * STRIDE[order[0]] + c1 * STRIDE[order[1]] + c2 * STRIDE[order[2]]
                for p in pieces(rows * 128):
                    cols = pl.ds(pl.multiple_of(block * SH + START[part] * 128 + p.start, 128), p.size)
                    dst[c0, c1, c2, :, p] = stage[0:1, cols].astype(jnp.float32)
                return carry

            lax.fori_loop(0, 4, body, 0)

    def halves(part):
        rows, cut = PARTS[part][1:3]
        return pl.ds(0, cut * 128), pl.ds(cut * 128, (rows - cut) * 128)

    def view(part, phase, c, half):
        ref = data[part][phase]
        return ref.at[c, pl.ds(2 * half, 2)] if phase < 2 else ref.at[c, :, halves(part)[half]]

    def landed(part, phase, kind, half):
        ref = landing[part][phase].at[kind]
        return ref if phase < 2 else ref.at[:, pl.ds(0, halves(part)[half].size)]

    HALF = {AP: 0, AM: 1, BP: 1, BM: 0, CP: 0, CM: 1}
    CHUNK = {AP: 2, AM: -2, BP: 1, BM: -1, CP: 1, CM: -1}

    def ring(part, phase, kind):
        axis = PARTS[part][0][phase]
        return pltpu.make_async_remote_copy(
            src_ref=view(part, phase, beside(axis, CHUNK[kind]), HALF[kind]),
            dst_ref=landed(part, phase, kind, HALF[kind]),
            send_sem=ring_send,
            recv_sem=ring_recv.at[RECV[part, phase, kind < BP]],
            device_id={axis: beside(axis, 1 if kind in (AP, BP, CP) else -1)},
            device_id_type=MESH,
        )

    def wait_bytes(ref, sem):
        pltpu.make_async_copy(ref, ref, sem).wait()

    def add_up(dst, *srcs):
        lead, width = dst.shape[:-2], dst.shape[-1]

        def one(idx):
            for p in pieces(width):
                at_p = idx + (slice(None), p)
                total = srcs[0][at_p]
                for s in srcs[1:]:
                    total = total + s[at_p]
                dst[at_p] = total

        if len(lead) == 2:

            def body(i, carry):
                for j in range(lead[0]):
                    one((j, i))
                return carry

            lax.fori_loop(0, lead[1], body, 0)
        else:
            for j in range(lead[0] if lead else 1):
                one((j,) if lead else ())

    def straight(part, phase, step):
        axis = PARTS[part][0][phase]
        there = beside(axis, step)
        return pltpu.make_async_remote_copy(
            src_ref=data[part][phase].at[there],
            dst_ref=landing[part][phase].at[step - 1],
            send_sem=ring_send,
            recv_sem=ring_recv.at[RECV[part, phase, False]],
            device_id={axis: there},
            device_id_type=MESH,
        )

    def is_straight(part, phase):
        return PARTS[part][3] and phase > 0

    def open_phase(part, phase):
        if is_straight(part, phase):
            for step in (2, 1, 3):
                straight(part, phase, step).start()
            return
        for kind in (AP, AM, BP, BM):
            ring(part, phase, kind).start()

    def forward(part, phase):
        if is_straight(part, phase):
            return
        axis = PARTS[part][0][phase]
        arrived = data[part][2].at[0] if phase == 2 else landing[part][phase].at[pl.ds(0, 2)]
        wait_bytes(arrived, ring_recv.at[RECV[part, phase, True]])
        for a, c in ((AP, CP), (AM, CM)):
            mine = view(part, phase, beside(axis, CHUNK[c]), HALF[c])
            add_up(mine, mine, landed(part, phase, a, HALF[a]))
            ring(part, phase, c).start()

    def close_phase(part, phase):
        axis = PARTS[part][0][phase]
        if is_straight(part, phase):
            arrived = landing[part][phase]
            wait_bytes(arrived, ring_recv.at[RECV[part, phase, False]])
            out = data[part][2] if phase == 1 else grads.at[:, pl.ds(START[part] * 128, PARTS[part][1] * 128)]
            add_up(out, data[part][phase].at[at[axis]], *[arrived.at[i] for i in range(3)])
            return
        last = data[part][2].at[pl.ds(0, 2)]
        wait_bytes(last if phase == 2 else landing[part][phase].at[pl.ds(2, 4)], ring_recv.at[RECV[part, phase, False]])
        for half, b, c in ((0, BM, CP), (1, BP, CM)):
            srcs = (
                view(part, phase, at[axis], half),
                landed(part, phase, b, half),
                landed(part, phase, c, half),
            )
            if phase < 2:
                add_up(data[part][phase + 1].at[pl.ds(2 * half, 2)], *srcs)
            else:
                cols = halves(part)[half]
                add_up(grads.at[:, pl.ds(START[part] * 128 + cols.start, cols.size)], *srcs)

    for n, part in enumerate(LOADING):
        axis = PARTS[part][0][0]
        for i in (groups[:1], groups[1:])[n] if n < 2 else ():
            loaded(i)
        convert(part, beside(axis, 2), 0)
        convert(part, beside(axis, 2), 1)
        if n == 0:
            pl.semaphore_wait(barrier, 8)
        ring(part, 0, AP).start()
        ring(part, 0, AM).start()
    for part in LOADING:
        axis = PARTS[part][0][0]
        convert(part, beside(axis, 1), 1)
        convert(part, beside(axis, -1), 0)
        if PARTS[part][3]:
            continue
        ring(part, 0, BP).start()
        ring(part, 0, BM).start()
    for part in LOADING:
        axis = PARTS[part][0][0]
        convert(part, beside(axis, 1), 0)
        convert(part, beside(axis, -1), 1)
    for part in ORDER_A:
        if PARTS[part][3]:
            ring(part, 0, BP).start()
            ring(part, 0, BM).start()
        forward(part, 0)
    for part in LOADING:
        axis = PARTS[part][0][0]
        convert(part, at[axis], 0)
        convert(part, at[axis], 1)

    def pair_copy(src, dst, n, axis):
        return pltpu.make_async_remote_copy(
            src_ref=src, dst_ref=dst, send_sem=rest_send, recv_sem=pair_recv.at[n],
            device_id={axis: 1 - at[axis]}, device_id_type=MESH,
        )

    wait_bytes(own, own_sem)
    shard_1 = pair_copy(own, cand.at[0], 0, "core")
    shard_2 = pair_copy(own, cand.at[2], 1, "zl")
    shard_3 = pair_copy(cand.at[2], cand.at[1], 0, "core")

    mine = at["zl"] * 2 + at["core"]
    partner_copy.wait()
    mate = partner[0, mine]
    apart = jnp.full((1, 1024), mine ^ mate, jnp.int32)
    is_one, is_two = apart == 1, apart == 2
    survive = jnp.full((1, 1024), mate - mine, jnp.int32) > 0

    def keep(a, cols, value, values):
        theirs = jnp.where(is_one, values[0], jnp.where(is_two, values[1], values[2]))
        state[a, 0:1, cols] = jnp.where(survive, value, 0.0)
        state[a, 1:2, cols] = jnp.where(survive, theirs, 0.0)

    def choose(i, carry):
        cols = pl.ds(pl.multiple_of(i * 1024, 1024), 1024)
        for a in range(3):
            keep(a, cols, own[a, :, cols], [cand[k, a, :, cols] for k in (0, 2, 1)])
        return carry

    def choose_grads(i, carry):
        cols = pl.ds(pl.multiple_of(i * 1024, 1024), 1024)
        keep(3, cols, grads[:, cols], [cand_g[k, :, cols] for k in (0, 2, 1)])
        return carry

    early = START[EARLY] * 128
    shares = (pl.ds(0, early), pl.ds(early, SH - early))

    def grads_copy(step, share):
        src = cand_g.at[2] if step == 2 else grads
        return pair_copy(
            src.at[:, shares[share]], cand_g.at[(0, 2, 1)[step], :, shares[share]], 2 + 2 * share + step % 2, ("core", "zl", "core")[step]
        )

    for phase in (0, 1, 2):
        for part in ORDER_LATER if phase else ORDER_SUM:
            close_phase(part, phase)
            if phase < 2:
                open_phase(part, phase + 1)
            elif part == [p for p in ORDER_LATER if p < EARLY][-1]:
                grads_copy(0, 0).start()
                grads_copy(1, 0).start()
            if phase == 0 and part == 1:
                shard_1.start()
                shard_2.start()
        if phase < 2:
            for part in ORDER_LATER:
                forward(part, phase + 1)
        if phase == 0:
            shard_2.wait_recv()
            shard_3.start()
        if phase == 1:
            wait_bytes(cand.at[pl.ds(0, 2)], pair_recv.at[0])
            lax.fori_loop(0, 16, choose, 0)

    def squares(i, total):
        tile = grads[:, pl.ds(pl.multiple_of(i * 1024, 1024), 1024)]
        return total + tile * tile

    total = lax.fori_loop(0, 16, squares, jnp.zeros((1, 1024), jnp.float32))
    near[0] = jnp.sum(total.reshape(8, 128), axis=0, keepdims=True)

    def spread(buf, k, ids, n):
        return pltpu.make_async_remote_copy(
            src_ref=buf.at[0], dst_ref=buf.at[k], send_sem=rest_send, recv_sem=norm_recv.at[n],
            device_id=ids[k], device_id_type=MESH,
        )

    for k in sorted(range(1, 16), key=lambda k: -min(k // 4, 4 - k // 4)):
        spread(near, k, near_ids, 0).start()
    grads_copy(0, 1).start()
    grads_copy(1, 1).start()
    grads_copy(1, 0).wait_recv()
    grads_copy(2, 0).start()
    wait_bytes(near.at[pl.ds(1, 15)], norm_recv.at[0])
    far[0] = functools.reduce(jnp.add, [near[k] for k in range(16)])
    for k in sorted(range(1, 16), key=lambda k: -(min(k // 4, 4 - k // 4) + min(k % 4, 4 - k % 4))):
        spread(far, k, far_ids, 1).start()
    grads_copy(1, 1).wait_recv()
    grads_copy(2, 1).start()
    for share in (0, 1):
        wait_bytes(cand_g.at[pl.ds(0, 2), :, shares[share]], pair_recv.at[2 + 2 * share])
    lax.fori_loop(0, 16, choose_grads, 0)

    wait_bytes(gauge.at[:, pl.ds(0, 63 * SH)], ring_send)
    wait_bytes(gauge.at[:, pl.ds(0, 12 * SH + 30 * 128)], rest_send)
    wait_bytes(far.at[pl.ds(1, 15)], norm_recv.at[1])
    squares_sum[...] = functools.reduce(jnp.add, [far[k] for k in range(16)])


def update_kernel(state, squares_sum, out_w, out_m, out_v, buf, sem):
    norm2 = jnp.sum(squares_sum[...], axis=1, keepdims=True)
    scale = 1.0 / jnp.maximum(jnp.sqrt(norm2 / (4 * N_DP * SH)), 1.0)
    outs = (out_w, out_m, out_v)
    n = SH // 4

    def copies(q):
        cols = pl.ds(pl.multiple_of(q * n, n), n)
        return [pltpu.make_async_copy(buf.at[a, :, cols], outs[a].at[0, 0, :, cols], sem.at[a]) for a in range(3)]

    def quarter(q, carry):
        for i in range(n // 512):
            cols = pl.ds(pl.multiple_of(q * n + i * 512, 512), 512)
            weights, first, second, total = [state[a, :, cols] for a in range(4)]
            scaled = scale * total
            first_new = beta_one * first + (1.0 - beta_one) * scaled
            second_new = beta_two * second + (1.0 - beta_two) * scaled * scaled
            change = first_new / bias_one / (jnp.sqrt(second_new / bias_two) + eps_value) + decay * weights
            buf[0, :, cols] = weights - rate * change
            buf[1, :, cols] = first_new
            buf[2, :, cols] = second_new
        for c in copies(q):
            c.start()
        return carry

    lax.fori_loop(0, 4, quarter, 0)
    for a in range(3):
        pltpu.make_async_copy(buf.at[a], outs[a].at[0, 0], sem.at[a]).wait()


def on_device(master, moment1, moment2, local_grad, partner):
    f32 = jnp.float32
    vmem = []
    for _, rows, cut, straight in PARTS:
        vmem += [pltpu.VMEM(n + (1, rows * 128), f32) for n in ((4, 4, 4), (4, 4), (4,), (6, 2, 4), (3, 4) if straight else (6, 2))]
        vmem.append(pltpu.VMEM((3, 1, rows * 128) if straight else (6, 1, max(cut, rows - cut) * 128), f32))
    dma = pltpu.SemaphoreType.DMA
    out = jax.ShapeDtypeStruct((1, 1, 2, SH), f32)
    state, squares_sum = pl.pallas_call(
        kernel,
        out_shape=(pltpu.VMEM((4, 2, SH), f32), pltpu.VMEM((1, 128), f32)),
        in_specs=[pl.BlockSpec(memory_space=pltpu.HBM)] * 5,
        out_specs=[pl.BlockSpec(memory_space=pltpu.VMEM)] * 2,
        scratch_shapes=[
            pltpu.VMEM((1, N_DP * SH), jnp.bfloat16),
            pltpu.VMEM((3, 1, SH), f32),
            pltpu.VMEM((3, 3, 1, SH), f32),
            pltpu.VMEM((1, SH), f32),
            pltpu.VMEM((3, 1, SH), f32),
            pltpu.VMEM((16, 1, 128), f32),
            pltpu.VMEM((16, 1, 128), f32),
            pltpu.VMEM((1, 63 * SH), f32),
        ]
        + [pltpu.SMEM((1, 4), jnp.int32), dma]
        + [dma((4,)), dma, dma, dma((len(RECV),)), dma, dma((6,)), dma((2,))]
        + vmem,
        compiler_params=pltpu.CompilerParams(collective_id=0, has_side_effects=True),
        name="step",
    )(partner, master, moment1, moment2, local_grad)
    return pl.pallas_call(
        update_kernel,
        out_shape=(out, out, out),
        in_specs=[pl.BlockSpec(memory_space=pltpu.VMEM)] * 2,
        out_specs=[pl.BlockSpec(memory_space=pltpu.HBM)] * 3,
        scratch_shapes=[pltpu.VMEM((3, 2, SH), f32), dma((3,))],
        name="update",
    )(*[pltpu.with_memory_space_constraint(v, pltpu.VMEM) for v in (state, squares_sum)])


def solution(mesh):
    finer = Mesh(mesh.devices.reshape(2, 2, 4, 4, 4), PAIR + DP)
    in_specs = (P(PAIR, DP), P(PAIR, DP), P(PAIR, DP), P(PAIR, DP, None), P(DP, None))
    out_specs = (P(PAIR, DP, None, None),) * 3
    return jax.shard_map(on_device, mesh=finer, in_specs=in_specs, out_specs=out_specs, check_vma=False)
```

```python
import functools

import jax
import jax.numpy as jnp
from jax import lax
from jax.experimental import pallas as pl
from jax.experimental.pallas import tpu as pltpu
from jax.sharding import Mesh
from jax.sharding import PartitionSpec as P

beta_one = 0.9
beta_two = 0.95
bias_one = 1.0 - 0.9**10
bias_two = 1.0 - 0.95**10
rate = 0.001
decay = 0.1
eps_value = 1e-08

SH = 16384
N_DP = 64
PAIR = ("zl", "core")
DP = ("zh", "x", "y")
STRIDE = {"zh": 16, "x": 4, "y": 1}
MESH = pl.DeviceIdType.MESH

XYZ, YXZ, ZXY, ZYX = ("x", "y", "zh"), ("y", "x", "zh"), ("zh", "x", "y"), ("zh", "y", "x")
PARTS = (
    (ZXY, 12, 8, (2,)),
    (ZYX, 12, 8, (2,)),
    (XYZ, 24, 12, (2,)),
    (YXZ, 24, 12, (2,)),
    (XYZ, 16, 8, (2,)),
    (YXZ, 16, 8, (2,)),
    (XYZ, 12, 8, (1, 2)),
    (YXZ, 12, 8, (1, 2)),
)
START = tuple(sum(p[1] for p in PARTS[:i]) for i in range(len(PARTS)))
LATE = (6, 7,)
EARLY = 6
LOADING = (2, 3, 0, 1) + tuple(range(4, len(PARTS)))
ORDER_A = (2,3,4,5,0,1,6,7)
ORDER_SUM = (2,3,0,1,4,5,6,7)
ORDER_LATER = (2,3,0,1,4,5,6,7)
AP, AM, BP, BM, CP, CM = range(6)
RECV = [(i, phase, a) for i, p in enumerate(PARTS) for phase in range(3) for a in (True, False) if not (a and phase in p[3])]
RECV = {key: n for n, key in enumerate(RECV)}


def kernel(
    partner_hbm, w_hbm, m_hbm, v_hbm, g_hbm, state, squares_sum,
    stage, own, cand, grads, cand_g, near, far,
    gauge, partner, partner_sem, load_sem, own_sem, ring_send, ring_recv, rest_send, pair_recv, norm_recv, *ring_bufs,
):
    data = [ring_bufs[6 * p : 6 * p + 3] for p in range(len(PARTS))]
    landing = [ring_bufs[6 * p + 3 : 6 * p + 6] for p in range(len(PARTS))]
    at = {a: lax.axis_index(a) for a in PAIR + DP}

    def beside(axis, step):
        return lax.rem(at[axis] + step + 4, 4)

    groups = (2, 1, -1, 0)
    for i in groups:
        for zh in range(4):
            cols = pl.ds((zh * 16 + beside("x", i) * 4) * SH, 4 * SH)
            pltpu.make_async_copy(g_hbm.at[0, :, cols], stage.at[:, cols], load_sem.at[i % 4]).start()
    for i, ref in enumerate((w_hbm, m_hbm, v_hbm)):
        pltpu.make_async_copy(ref, own.at[i], own_sem).start()

    partner_copy = pltpu.make_async_copy(partner_hbm, partner, partner_sem)
    partner_copy.start()

    def loaded(i):
        part_of = stage.at[:, pl.ds(0, 16 * SH)]
        pltpu.make_async_copy(part_of, part_of, load_sem.at[i % 4]).wait()

    barrier = pltpu.get_barrier_semaphore()
    near_ids = [
        {"zh": beside("zh", k // 4), "zl": lax.rem(at["zl"] + (k // 2) % 2, 2), "core": lax.rem(at["core"] + k % 2, 2)}
        for k in range(16)
    ]
    far_ids = [{"x": beside("x", k // 4), "y": beside("y", k % 4)} for k in range(16)]
    for axis in DP:
        for step in (1, -1):
            pl.semaphore_signal(barrier, inc=1, device_id={axis: beside(axis, step)}, device_id_type=MESH)
    for axis in PAIR:
        pl.semaphore_signal(barrier, inc=1, device_id={axis: 1 - at[axis]}, device_id_type=MESH)

    def pieces(width):
        return [pl.ds(lo, min(1024, width - lo)) for lo in range(0, width, 1024)]

    def convert(part, c0, half):
        order, rows = PARTS[part][:2]
        dst = data[part][0]
        for c1 in (2 * half, 2 * half + 1):

            def body(c2, carry, c1=c1):
                block = c0 * STRIDE[order[0]] + c1 * STRIDE[order[1]] + c2 * STRIDE[order[2]]
                for p in pieces(rows * 128):
                    cols = pl.ds(pl.multiple_of(block * SH + START[part] * 128 + p.start, 128), p.size)
                    dst[c0, c1, c2, :, p] = stage[0:1, cols].astype(jnp.float32)
                return carry

            lax.fori_loop(0, 4, body, 0)

    def halves(part):
        rows, cut = PARTS[part][1:3]
        return pl.ds(0, cut * 128), pl.ds(cut * 128, (rows - cut) * 128)

    def view(part, phase, c, half):
        ref = data[part][phase]
        return ref.at[c, pl.ds(2 * half, 2)] if phase < 2 else ref.at[c, :, halves(part)[half]]

    def landed(part, phase, kind, half):
        ref = landing[part][phase].at[kind]
        return ref if phase < 2 else ref.at[:, pl.ds(0, halves(part)[half].size)]

    HALF = {AP: 0, AM: 1, BP: 1, BM: 0, CP: 0, CM: 1}
    CHUNK = {AP: 2, AM: -2, BP: 1, BM: -1, CP: 1, CM: -1}

    def ring(part, phase, kind):
        axis = PARTS[part][0][phase]
        return pltpu.make_async_remote_copy(
            src_ref=view(part, phase, beside(axis, CHUNK[kind]), HALF[kind]),
            dst_ref=landed(part, phase, kind, HALF[kind]),
            send_sem=ring_send,
            recv_sem=ring_recv.at[RECV[part, phase, kind < BP]],
            device_id={axis: beside(axis, 1 if kind in (AP, BP, CP) else -1)},
            device_id_type=MESH,
        )

    def wait_bytes(ref, sem):
        pltpu.make_async_copy(ref, ref, sem).wait()

    def add_up(dst, *srcs):
        lead, width = dst.shape[:-2], dst.shape[-1]

        def one(idx):
            for p in pieces(width):
                at_p = idx + (slice(None), p)
                total = srcs[0][at_p]
                for s in srcs[1:]:
                    total = total + s[at_p]
                dst[at_p] = total

        if len(lead) == 2:

            def body(i, carry):
                for j in range(lead[0]):
                    one((j, i))
                return carry

            lax.fori_loop(0, lead[1], body, 0)
        else:
            for j in range(lead[0] if lead else 1):
                one((j,) if lead else ())

    def straight(part, phase, step):
        axis = PARTS[part][0][phase]
        there = beside(axis, step)
        return pltpu.make_async_remote_copy(
            src_ref=data[part][phase].at[there],
            dst_ref=landing[part][phase].at[step - 1],
            send_sem=ring_send,
            recv_sem=ring_recv.at[RECV[part, phase, False]],
            device_id={axis: there},
            device_id_type=MESH,
        )

    def is_straight(part, phase):
        return phase in PARTS[part][3]

    def open_phase(part, phase):
        if is_straight(part, phase):
            for step in (2, 1, 3):
                straight(part, phase, step).start()
            return
        for kind in (AP, AM, BP, BM):
            ring(part, phase, kind).start()

    def forward(part, phase):
        if is_straight(part, phase):
            return
        axis = PARTS[part][0][phase]
        arrived = data[part][2].at[0] if phase == 2 else landing[part][phase].at[pl.ds(0, 2)]
        wait_bytes(arrived, ring_recv.at[RECV[part, phase, True]])
        for a, c in ((AP, CP), (AM, CM)):
            mine = view(part, phase, beside(axis, CHUNK[c]), HALF[c])
            add_up(mine, mine, landed(part, phase, a, HALF[a]))
            ring(part, phase, c).start()

    def close_phase(part, phase):
        axis = PARTS[part][0][phase]
        if is_straight(part, phase):
            arrived = landing[part][phase]
            wait_bytes(arrived, ring_recv.at[RECV[part, phase, False]])
            out = data[part][2] if phase == 1 else grads.at[:, pl.ds(START[part] * 128, PARTS[part][1] * 128)]
            add_up(out, data[part][phase].at[at[axis]], *[arrived.at[i] for i in range(3)])
            return
        last = data[part][2].at[pl.ds(0, 2)]
        wait_bytes(last if phase == 2 else landing[part][phase].at[pl.ds(2, 4)], ring_recv.at[RECV[part, phase, False]])
        for half, b, c in ((0, BM, CP), (1, BP, CM)):
            srcs = (
                view(part, phase, at[axis], half),
                landed(part, phase, b, half),
                landed(part, phase, c, half),
            )
            if phase < 2:
                add_up(data[part][phase + 1].at[pl.ds(2 * half, 2)], *srcs)
            else:
                cols = halves(part)[half]
                add_up(grads.at[:, pl.ds(START[part] * 128 + cols.start, cols.size)], *srcs)

    for n, part in enumerate(LOADING):
        axis = PARTS[part][0][0]
        for i in (groups[:1], groups[1:])[n] if n < 2 else ():
            loaded(i)
        convert(part, beside(axis, 2), 0)
        convert(part, beside(axis, 2), 1)
        if n == 0:
            pl.semaphore_wait(barrier, 8)
        ring(part, 0, AP).start()
        ring(part, 0, AM).start()
    for part in LOADING:
        axis = PARTS[part][0][0]
        convert(part, beside(axis, 1), 1)
        convert(part, beside(axis, -1), 0)
        if part in LATE:
            continue
        ring(part, 0, BP).start()
        ring(part, 0, BM).start()
    for part in LOADING:
        axis = PARTS[part][0][0]
        convert(part, beside(axis, 1), 0)
        convert(part, beside(axis, -1), 1)
    for part in ORDER_A:
        if part in LATE:
            ring(part, 0, BP).start()
            ring(part, 0, BM).start()
        forward(part, 0)
    for part in LOADING:
        axis = PARTS[part][0][0]
        convert(part, at[axis], 0)
        convert(part, at[axis], 1)

    def pair_copy(src, dst, n, axis):
        return pltpu.make_async_remote_copy(
            src_ref=src, dst_ref=dst, send_sem=rest_send, recv_sem=pair_recv.at[n],
            device_id={axis: 1 - at[axis]}, device_id_type=MESH,
        )

    wait_bytes(own, own_sem)
    shard_1 = pair_copy(own, cand.at[0], 0, "core")
    shard_2 = pair_copy(own, cand.at[2], 1, "zl")
    shard_3 = pair_copy(cand.at[2], cand.at[1], 0, "core")

    mine = at["zl"] * 2 + at["core"]
    partner_copy.wait()
    mate = partner[0, mine]
    apart = jnp.full((1, 1024), mine ^ mate, jnp.int32)
    is_one, is_two = apart == 1, apart == 2
    survive = jnp.full((1, 1024), mate - mine, jnp.int32) > 0

    def keep(a, cols, value, values):
        theirs = jnp.where(is_one, values[0], jnp.where(is_two, values[1], values[2]))
        state[a, 0:1, cols] = jnp.where(survive, value, 0.0)
        state[a, 1:2, cols] = jnp.where(survive, theirs, 0.0)

    def choose(i, carry):
        cols = pl.ds(pl.multiple_of(i * 1024, 1024), 1024)
        for a in range(3):
            keep(a, cols, own[a, :, cols], [cand[k, a, :, cols] for k in (0, 2, 1)])
        return carry

    def choose_grads(i, carry):
        cols = pl.ds(pl.multiple_of(i * 1024, 1024), 1024)
        keep(3, cols, grads[:, cols], [cand_g[k, :, cols] for k in (0, 2, 1)])
        return carry

    early = START[EARLY] * 128
    shares = (pl.ds(0, early), pl.ds(early, SH - early))

    def grads_copy(step, share):
        src = cand_g.at[2] if step == 2 else grads
        return pair_copy(
            src.at[:, shares[share]], cand_g.at[(0, 2, 1)[step], :, shares[share]], 2 + 2 * share + step % 2, ("core", "zl", "core")[step]
        )

    for phase in (0, 1, 2):
        for part in ORDER_LATER if phase else ORDER_SUM:
            close_phase(part, phase)
            if phase < 2:
                open_phase(part, phase + 1)
            elif part == [p for p in ORDER_LATER if p < EARLY][-1]:
                grads_copy(0, 0).start()
                grads_copy(1, 0).start()
            if phase == 0 and part == 1:
                shard_1.start()
                shard_2.start()
        if phase < 2:
            for part in ORDER_LATER:
                forward(part, phase + 1)
        if phase == 0:
            shard_2.wait_recv()
            shard_3.start()
        if phase == 1:
            wait_bytes(cand.at[pl.ds(0, 2)], pair_recv.at[0])
            lax.fori_loop(0, 16, choose, 0)

    def squares(i, total):
        tile = grads[:, pl.ds(pl.multiple_of(i * 1024, 1024), 1024)]
        return total + tile * tile

    total = lax.fori_loop(0, 16, squares, jnp.zeros((1, 1024), jnp.float32))
    near[0] = jnp.sum(total.reshape(8, 128), axis=0, keepdims=True)

    def spread(buf, k, ids, n):
        return pltpu.make_async_remote_copy(
            src_ref=buf.at[0], dst_ref=buf.at[k], send_sem=rest_send, recv_sem=norm_recv.at[n],
            device_id=ids[k], device_id_type=MESH,
        )

    for k in sorted(range(1, 16), key=lambda k: -min(k // 4, 4 - k // 4)):
        spread(near, k, near_ids, 0).start()
    grads_copy(0, 1).start()
    grads_copy(1, 1).start()
    grads_copy(1, 0).wait_recv()
    grads_copy(2, 0).start()
    wait_bytes(near.at[pl.ds(1, 15)], norm_recv.at[0])
    far[0] = functools.reduce(jnp.add, [near[k] for k in range(16)])
    for k in sorted(range(1, 16), key=lambda k: -(min(k // 4, 4 - k // 4) + min(k % 4, 4 - k % 4))):
        spread(far, k, far_ids, 1).start()
    grads_copy(1, 1).wait_recv()
    grads_copy(2, 1).start()
    for share in (0, 1):
        wait_bytes(cand_g.at[pl.ds(0, 2), :, shares[share]], pair_recv.at[2 + 2 * share])
    lax.fori_loop(0, 16, choose_grads, 0)

    wait_bytes(gauge.at[:, pl.ds(0, 63 * SH)], ring_send)
    wait_bytes(gauge.at[:, pl.ds(0, 12 * SH + 30 * 128)], rest_send)
    wait_bytes(far.at[pl.ds(1, 15)], norm_recv.at[1])
    squares_sum[...] = functools.reduce(jnp.add, [far[k] for k in range(16)])


def update_kernel(state, squares_sum, out_w, out_m, out_v, buf, sem):
    norm2 = jnp.sum(squares_sum[...], axis=1, keepdims=True)
    scale = 1.0 / jnp.maximum(jnp.sqrt(norm2 / (4 * N_DP * SH)), 1.0)
    outs = (out_w, out_m, out_v)
    n = SH // 4

    def copies(q):
        cols = pl.ds(pl.multiple_of(q * n, n), n)
        return [pltpu.make_async_copy(buf.at[a, :, cols], outs[a].at[0, 0, :, cols], sem.at[a]) for a in range(3)]

    def quarter(q, carry):
        for i in range(n // 512):
            cols = pl.ds(pl.multiple_of(q * n + i * 512, 512), 512)
            weights, first, second, total = [state[a, :, cols] for a in range(4)]
            scaled = scale * total
            first_new = beta_one * first + (1.0 - beta_one) * scaled
            second_new = beta_two * second + (1.0 - beta_two) * scaled * scaled
            change = first_new * (1.0 / bias_one) / (jnp.sqrt(second_new * (1.0 / bias_two)) + eps_value) + decay * weights
            buf[0, :, cols] = weights - rate * change
            buf[1, :, cols] = first_new
            buf[2, :, cols] = second_new
        for c in copies(q):
            c.start()
        return carry

    lax.fori_loop(0, 4, quarter, 0)
    for a in range(3):
        pltpu.make_async_copy(buf.at[a], outs[a].at[0, 0], sem.at[a]).wait()


def on_device(master, moment1, moment2, local_grad, partner):
    f32 = jnp.float32
    vmem = []
    for _, rows, cut, straight in PARTS:
        vmem += [pltpu.VMEM(n + (1, rows * 128), f32) for n in ((4, 4, 4), (4, 4), (4,), (6, 2, 4), (3, 4) if 1 in straight else (6, 2))]
        vmem.append(pltpu.VMEM((3, 1, rows * 128) if 2 in straight else (6, 1, max(cut, rows - cut) * 128), f32))
    dma = pltpu.SemaphoreType.DMA
    out = jax.ShapeDtypeStruct((1, 1, 2, SH), f32)
    state, squares_sum = pl.pallas_call(
        kernel,
        out_shape=(pltpu.VMEM((4, 2, SH), f32), pltpu.VMEM((1, 128), f32)),
        in_specs=[pl.BlockSpec(memory_space=pltpu.HBM)] * 5,
        out_specs=[pl.BlockSpec(memory_space=pltpu.VMEM)] * 2,
        scratch_shapes=[
            pltpu.VMEM((1, N_DP * SH), jnp.bfloat16),
            pltpu.VMEM((3, 1, SH), f32),
            pltpu.VMEM((3, 3, 1, SH), f32),
            pltpu.VMEM((1, SH), f32),
            pltpu.VMEM((3, 1, SH), f32),
            pltpu.VMEM((16, 1, 128), f32),
            pltpu.VMEM((16, 1, 128), f32),
            pltpu.VMEM((1, 63 * SH), f32),
        ]
        + [pltpu.SMEM((1, 4), jnp.int32), dma]
        + [dma((4,)), dma, dma, dma((len(RECV),)), dma, dma((6,)), dma((2,))]
        + vmem,
        compiler_params=pltpu.CompilerParams(collective_id=0, has_side_effects=True),
        name="step",
    )(partner, master, moment1, moment2, local_grad)
    return pl.pallas_call(
        update_kernel,
        out_shape=(out, out, out),
        in_specs=[pl.BlockSpec(memory_space=pltpu.VMEM)] * 2,
        out_specs=[pl.BlockSpec(memory_space=pltpu.HBM)] * 3,
        scratch_shapes=[pltpu.VMEM((3, 2, SH), f32), dma((3,))],
        name="update",
    )(*[pltpu.with_memory_space_constraint(v, pltpu.VMEM) for v in (state, squares_sum)])


def solution(mesh):
    finer = Mesh(mesh.devices.reshape(2, 2, 4, 4, 4), PAIR + DP)
    in_specs = (P(PAIR, DP), P(PAIR, DP), P(PAIR, DP), P(PAIR, DP, None), P(DP, None))
    out_specs = (P(PAIR, DP, None, None),) * 3
    return jax.shard_map(on_device, mesh=finer, in_specs=in_specs, out_specs=out_specs, check_vma=False)
```

```python
import functools

import jax
import jax.numpy as jnp
from jax import lax
from jax.experimental import pallas as pl
from jax.experimental.pallas import tpu as pltpu
from jax.sharding import Mesh
from jax.sharding import PartitionSpec as P

beta_one = 0.9
beta_two = 0.95
bias_one = 1.0 - 0.9**10
bias_two = 1.0 - 0.95**10
rate = 0.001
decay = 0.1
eps_value = 1e-08

SH = 16384
N_DP = 64
PAIR = ("zl", "core")
DP = ("zh", "x", "y")
STRIDE = {"zh": 16, "x": 4, "y": 1}
MESH = pl.DeviceIdType.MESH

XYZ, YXZ, ZXY, ZYX = ("x", "y", "zh"), ("y", "x", "zh"), ("zh", "x", "y"), ("zh", "y", "x")
PARTS = (
    (ZXY, 12, 8, (2,)),
    (ZYX, 12, 8, (2,)),
    (XYZ, 28, 16, (2,)),
    (YXZ, 28, 16, (2,)),
    (XYZ, 12, 8, (1, 2)),
    (YXZ, 12, 8, (1, 2)),
    (XYZ, 12, 8, (1, 2)),
    (YXZ, 12, 8, (1, 2)),
)
START = tuple(sum(p[1] for p in PARTS[:i]) for i in range(len(PARTS)))
LATE = (6, 7,)
EARLY = 6
LOADING = (2, 3, 0, 1) + tuple(range(4, len(PARTS)))
ORDER_A = (2,3,4,5,0,1,6,7)
ORDER_SUM = (2,3,0,1,4,5,6,7)
ORDER_LATER = (2,3,0,1,4,5,6,7)
AP, AM, BP, BM, CP, CM = range(6)
RECV = [(i, phase, a) for i, p in enumerate(PARTS) for phase in range(3) for a in (True, False) if not (a and phase in p[3])]
RECV = {key: n for n, key in enumerate(RECV)}


def kernel(
    partner_hbm, w_hbm, m_hbm, v_hbm, g_hbm, state, squares_sum,
    stage, own, cand, grads, cand_g, near, far,
    gauge, partner, partner_sem, load_sem, own_sem, ring_send, ring_recv, rest_send, pair_recv, norm_recv, *ring_bufs,
):
    data = [ring_bufs[6 * p : 6 * p + 3] for p in range(len(PARTS))]
    landing = [ring_bufs[6 * p + 3 : 6 * p + 6] for p in range(len(PARTS))]
    at = {a: lax.axis_index(a) for a in PAIR + DP}

    def beside(axis, step):
        return lax.rem(at[axis] + step + 4, 4)

    groups = (2, 1, -1, 0)
    for i in groups:
        for zh in range(4):
            cols = pl.ds((zh * 16 + beside("x", i) * 4) * SH, 4 * SH)
            pltpu.make_async_copy(g_hbm.at[0, :, cols], stage.at[:, cols], load_sem.at[i % 4]).start()
    for i, ref in enumerate((w_hbm, m_hbm, v_hbm)):
        pltpu.make_async_copy(ref, own.at[i], own_sem).start()

    partner_copy = pltpu.make_async_copy(partner_hbm, partner, partner_sem)
    partner_copy.start()

    def loaded(i):
        part_of = stage.at[:, pl.ds(0, 16 * SH)]
        pltpu.make_async_copy(part_of, part_of, load_sem.at[i % 4]).wait()

    barrier = pltpu.get_barrier_semaphore()
    near_ids = [
        {"zh": beside("zh", k // 4), "zl": lax.rem(at["zl"] + (k // 2) % 2, 2), "core": lax.rem(at["core"] + k % 2, 2)}
        for k in range(16)
    ]
    far_ids = [{"x": beside("x", k // 4), "y": beside("y", k % 4)} for k in range(16)]
    for axis in DP:
        for step in (1, -1):
            pl.semaphore_signal(barrier, inc=1, device_id={axis: beside(axis, step)}, device_id_type=MESH)
    for axis in PAIR:
        pl.semaphore_signal(barrier, inc=1, device_id={axis: 1 - at[axis]}, device_id_type=MESH)

    def pieces(width):
        return [pl.ds(lo, min(1024, width - lo)) for lo in range(0, width, 1024)]

    def convert(part, c0, half):
        order, rows = PARTS[part][:2]
        dst = data[part][0]
        for c1 in (2 * half, 2 * half + 1):

            def body(c2, carry, c1=c1):
                block = c0 * STRIDE[order[0]] + c1 * STRIDE[order[1]] + c2 * STRIDE[order[2]]
                for p in pieces(rows * 128):
                    cols = pl.ds(pl.multiple_of(block * SH + START[part] * 128 + p.start, 128), p.size)
                    dst[c0, c1, c2, :, p] = stage[0:1, cols].astype(jnp.float32)
                return carry

            lax.fori_loop(0, 4, body, 0)

    def halves(part):
        rows, cut = PARTS[part][1:3]
        return pl.ds(0, cut * 128), pl.ds(cut * 128, (rows - cut) * 128)

    def view(part, phase, c, half):
        ref = data[part][phase]
        return ref.at[c, pl.ds(2 * half, 2)] if phase < 2 else ref.at[c, :, halves(part)[half]]

    def landed(part, phase, kind, half):
        ref = landing[part][phase].at[kind]
        return ref if phase < 2 else ref.at[:, pl.ds(0, halves(part)[half].size)]

    HALF = {AP: 0, AM: 1, BP: 1, BM: 0, CP: 0, CM: 1}
    CHUNK = {AP: 2, AM: -2, BP: 1, BM: -1, CP: 1, CM: -1}

    def ring(part, phase, kind):
        axis = PARTS[part][0][phase]
        return pltpu.make_async_remote_copy(
            src_ref=view(part, phase, beside(axis, CHUNK[kind]), HALF[kind]),
            dst_ref=landed(part, phase, kind, HALF[kind]),
            send_sem=ring_send,
            recv_sem=ring_recv.at[RECV[part, phase, kind < BP]],
            device_id={axis: beside(axis, 1 if kind in (AP, BP, CP) else -1)},
            device_id_type=MESH,
        )

    def wait_bytes(ref, sem):
        pltpu.make_async_copy(ref, ref, sem).wait()

    def add_up(dst, *srcs):
        lead, width = dst.shape[:-2], dst.shape[-1]

        def one(idx):
            for p in pieces(width):
                at_p = idx + (slice(None), p)
                total = srcs[0][at_p]
                for s in srcs[1:]:
                    total = total + s[at_p]
                dst[at_p] = total

        if len(lead) == 2:

            def body(i, carry):
                for j in range(lead[0]):
                    one((j, i))
                return carry

            lax.fori_loop(0, lead[1], body, 0)
        else:
            for j in range(lead[0] if lead else 1):
                one((j,) if lead else ())

    def straight(part, phase, step):
        axis = PARTS[part][0][phase]
        there = beside(axis, step)
        return pltpu.make_async_remote_copy(
            src_ref=data[part][phase].at[there],
            dst_ref=landing[part][phase].at[step - 1],
            send_sem=ring_send,
            recv_sem=ring_recv.at[RECV[part, phase, False]],
            device_id={axis: there},
            device_id_type=MESH,
        )

    def is_straight(part, phase):
        return phase in PARTS[part][3]

    def open_phase(part, phase):
        if is_straight(part, phase):
            for step in (2, 1, 3):
                straight(part, phase, step).start()
            return
        for kind in (AP, AM, BP, BM):
            ring(part, phase, kind).start()

    def forward(part, phase):
        if is_straight(part, phase):
            return
        axis = PARTS[part][0][phase]
        arrived = data[part][2].at[0] if phase == 2 else landing[part][phase].at[pl.ds(0, 2)]
        wait_bytes(arrived, ring_recv.at[RECV[part, phase, True]])
        for a, c in ((AP, CP), (AM, CM)):
            mine = view(part, phase, beside(axis, CHUNK[c]), HALF[c])
            add_up(mine, mine, landed(part, phase, a, HALF[a]))
            ring(part, phase, c).start()

    def close_phase(part, phase):
        axis = PARTS[part][0][phase]
        if is_straight(part, phase):
            arrived = landing[part][phase]
            wait_bytes(arrived, ring_recv.at[RECV[part, phase, False]])
            out = data[part][2] if phase == 1 else grads.at[:, pl.ds(START[part] * 128, PARTS[part][1] * 128)]
            add_up(out, data[part][phase].at[at[axis]], *[arrived.at[i] for i in range(3)])
            return
        last = data[part][2].at[pl.ds(0, 2)]
        wait_bytes(last if phase == 2 else landing[part][phase].at[pl.ds(2, 4)], ring_recv.at[RECV[part, phase, False]])
        for half, b, c in ((0, BM, CP), (1, BP, CM)):
            srcs = (
                view(part, phase, at[axis], half),
                landed(part, phase, b, half),
                landed(part, phase, c, half),
            )
            if phase < 2:
                add_up(data[part][phase + 1].at[pl.ds(2 * half, 2)], *srcs)
            else:
                cols = halves(part)[half]
                add_up(grads.at[:, pl.ds(START[part] * 128 + cols.start, cols.size)], *srcs)

    for n, part in enumerate(LOADING):
        axis = PARTS[part][0][0]
        for i in (groups[:1], groups[1:])[n] if n < 2 else ():
            loaded(i)
        convert(part, beside(axis, 2), 0)
        convert(part, beside(axis, 2), 1)
        if n == 0:
            pl.semaphore_wait(barrier, 8)
        ring(part, 0, AP).start()
        ring(part, 0, AM).start()
    for part in LOADING:
        axis = PARTS[part][0][0]
        convert(part, beside(axis, 1), 1)
        convert(part, beside(axis, -1), 0)
        if part in LATE:
            continue
        ring(part, 0, BP).start()
        ring(part, 0, BM).start()
    for part in LOADING:
        axis = PARTS[part][0][0]
        convert(part, beside(axis, 1), 0)
        convert(part, beside(axis, -1), 1)
    for part in ORDER_A:
        if part in LATE:
            ring(part, 0, BP).start()
            ring(part, 0, BM).start()
        forward(part, 0)
    for part in LOADING:
        axis = PARTS[part][0][0]
        convert(part, at[axis], 0)
        convert(part, at[axis], 1)

    def pair_copy(src, dst, n, axis):
        return pltpu.make_async_remote_copy(
            src_ref=src, dst_ref=dst, send_sem=rest_send, recv_sem=pair_recv.at[n],
            device_id={axis: 1 - at[axis]}, device_id_type=MESH,
        )

    wait_bytes(own, own_sem)
    shard_1 = pair_copy(own, cand.at[0], 0, "core")
    shard_2 = pair_copy(own, cand.at[2], 1, "zl")
    shard_3 = pair_copy(cand.at[2], cand.at[1], 0, "core")

    mine = at["zl"] * 2 + at["core"]
    partner_copy.wait()
    mate = partner[0, mine]
    apart = jnp.full((1, 1024), mine ^ mate, jnp.int32)
    is_one, is_two = apart == 1, apart == 2
    survive = jnp.full((1, 1024), mate - mine, jnp.int32) > 0

    def keep(a, cols, value, values):
        theirs = jnp.where(is_one, values[0], jnp.where(is_two, values[1], values[2]))
        state[a, 0:1, cols] = jnp.where(survive, value, 0.0)
        state[a, 1:2, cols] = jnp.where(survive, theirs, 0.0)

    def choose(i, carry):
        cols = pl.ds(pl.multiple_of(i * 1024, 1024), 1024)
        for a in range(3):
            keep(a, cols, own[a, :, cols], [cand[k, a, :, cols] for k in (0, 2, 1)])
        return carry

    def choose_grads(i, carry):
        cols = pl.ds(pl.multiple_of(i * 1024, 1024), 1024)
        keep(3, cols, grads[:, cols], [cand_g[k, :, cols] for k in (0, 2, 1)])
        return carry

    early = START[EARLY] * 128
    shares = (pl.ds(0, early), pl.ds(early, SH - early))

    def grads_copy(step, share):
        src = cand_g.at[2] if step == 2 else grads
        return pair_copy(
            src.at[:, shares[share]], cand_g.at[(0, 2, 1)[step], :, shares[share]], 2 + 2 * share + step % 2, ("core", "zl", "core")[step]
        )

    for phase in (0, 1, 2):
        for part in ORDER_LATER if phase else ORDER_SUM:
            close_phase(part, phase)
            if phase < 2:
                open_phase(part, phase + 1)
            elif part == [p for p in ORDER_LATER if p < EARLY][-1]:
                grads_copy(0, 0).start()
                grads_copy(1, 0).start()
            if phase == 0 and part == 1:
                shard_1.start()
                shard_2.start()
        if phase < 2:
            for part in ORDER_LATER:
                forward(part, phase + 1)
        if phase == 0:
            shard_2.wait_recv()
            shard_3.start()
        if phase == 1:
            wait_bytes(cand.at[pl.ds(0, 2)], pair_recv.at[0])
            lax.fori_loop(0, 16, choose, 0)

    def squares(i, total):
        tile = grads[:, pl.ds(pl.multiple_of(i * 1024, 1024), 1024)]
        return total + tile * tile

    total = lax.fori_loop(0, 16, squares, jnp.zeros((1, 1024), jnp.float32))
    near[0] = jnp.sum(total.reshape(8, 128), axis=0, keepdims=True)

    def spread(buf, k, ids, n):
        return pltpu.make_async_remote_copy(
            src_ref=buf.at[0], dst_ref=buf.at[k], send_sem=rest_send, recv_sem=norm_recv.at[n],
            device_id=ids[k], device_id_type=MESH,
        )

    for k in sorted(range(1, 16), key=lambda k: -min(k // 4, 4 - k // 4)):
        spread(near, k, near_ids, 0).start()
    grads_copy(0, 1).start()
    grads_copy(1, 1).start()
    grads_copy(1, 0).wait_recv()
    grads_copy(2, 0).start()
    wait_bytes(near.at[pl.ds(1, 15)], norm_recv.at[0])
    far[0] = functools.reduce(jnp.add, [near[k] for k in range(16)])
    for k in sorted(range(1, 16), key=lambda k: -(min(k // 4, 4 - k // 4) + min(k % 4, 4 - k % 4))):
        spread(far, k, far_ids, 1).start()
    grads_copy(1, 1).wait_recv()
    grads_copy(2, 1).start()
    for share in (0, 1):
        wait_bytes(cand_g.at[pl.ds(0, 2), :, shares[share]], pair_recv.at[2 + 2 * share])
    lax.fori_loop(0, 16, choose_grads, 0)

    wait_bytes(gauge.at[:, pl.ds(0, 63 * SH)], ring_send)
    wait_bytes(gauge.at[:, pl.ds(0, 12 * SH + 30 * 128)], rest_send)
    wait_bytes(far.at[pl.ds(1, 15)], norm_recv.at[1])
    squares_sum[...] = functools.reduce(jnp.add, [far[k] for k in range(16)])


def update_kernel(state, squares_sum, out_w, out_m, out_v, buf, sem):
    norm2 = jnp.sum(squares_sum[...], axis=1, keepdims=True)
    scale = 1.0 / jnp.maximum(jnp.sqrt(norm2 / (4 * N_DP * SH)), 1.0)
    outs = (out_w, out_m, out_v)
    n = SH // 4

    def copies(q):
        cols = pl.ds(pl.multiple_of(q * n, n), n)
        return [pltpu.make_async_copy(buf.at[a, :, cols], outs[a].at[0, 0, :, cols], sem.at[a]) for a in range(3)]

    def quarter(q, carry):
        for i in range(n // 512):
            cols = pl.ds(pl.multiple_of(q * n + i * 512, 512), 512)
            weights, first, second, total = [state[a, :, cols] for a in range(4)]
            scaled = scale * total
            first_new = beta_one * first + (1.0 - beta_one) * scaled
            second_new = beta_two * second + (1.0 - beta_two) * scaled * scaled
            change = first_new * (1.0 / bias_one) / (jnp.sqrt(second_new * (1.0 / bias_two)) + eps_value) + decay * weights
            buf[0, :, cols] = weights - rate * change
            buf[1, :, cols] = first_new
            buf[2, :, cols] = second_new
        for c in copies(q):
            c.start()
        return carry

    lax.fori_loop(0, 4, quarter, 0)
    for a in range(3):
        pltpu.make_async_copy(buf.at[a], outs[a].at[0, 0], sem.at[a]).wait()


def on_device(master, moment1, moment2, local_grad, partner):
    f32 = jnp.float32
    vmem = []
    for _, rows, cut, straight in PARTS:
        vmem += [pltpu.VMEM(n + (1, rows * 128), f32) for n in ((4, 4, 4), (4, 4), (4,), (6, 2, 4), (3, 4) if 1 in straight else (6, 2))]
        vmem.append(pltpu.VMEM((3, 1, rows * 128) if 2 in straight else (6, 1, max(cut, rows - cut) * 128), f32))
    dma = pltpu.SemaphoreType.DMA
    out = jax.ShapeDtypeStruct((1, 1, 2, SH), f32)
    state, squares_sum = pl.pallas_call(
        kernel,
        out_shape=(pltpu.VMEM((4, 2, SH), f32), pltpu.VMEM((1, 128), f32)),
        in_specs=[pl.BlockSpec(memory_space=pltpu.HBM)] * 5,
        out_specs=[pl.BlockSpec(memory_space=pltpu.VMEM)] * 2,
        scratch_shapes=[
            pltpu.VMEM((1, N_DP * SH), jnp.bfloat16),
            pltpu.VMEM((3, 1, SH), f32),
            pltpu.VMEM((3, 3, 1, SH), f32),
            pltpu.VMEM((1, SH), f32),
            pltpu.VMEM((3, 1, SH), f32),
            pltpu.VMEM((16, 1, 128), f32),
            pltpu.VMEM((16, 1, 128), f32),
            pltpu.VMEM((1, 63 * SH), f32),
        ]
        + [pltpu.SMEM((1, 4), jnp.int32), dma]
        + [dma((4,)), dma, dma, dma((len(RECV),)), dma, dma((6,)), dma((2,))]
        + vmem,
        compiler_params=pltpu.CompilerParams(collective_id=0, has_side_effects=True),
        name="step",
    )(partner, master, moment1, moment2, local_grad)
    return pl.pallas_call(
        update_kernel,
        out_shape=(out, out, out),
        in_specs=[pl.BlockSpec(memory_space=pltpu.VMEM)] * 2,
        out_specs=[pl.BlockSpec(memory_space=pltpu.HBM)] * 3,
        scratch_shapes=[pltpu.VMEM((3, 2, SH), f32), dma((3,))],
        name="update",
    )(*[pltpu.with_memory_space_constraint(v, pltpu.VMEM) for v in (state, squares_sum)])


def solution(mesh):
    finer = Mesh(mesh.devices.reshape(2, 2, 4, 4, 4), PAIR + DP)
    in_specs = (P(PAIR, DP), P(PAIR, DP), P(PAIR, DP), P(PAIR, DP, None), P(DP, None))
    out_specs = (P(PAIR, DP, None, None),) * 3
    return jax.shard_map(on_device, mesh=finer, in_specs=in_specs, out_specs=out_specs, check_vma=False)
```

```python
import functools

import jax
import jax.numpy as jnp
from jax import lax
from jax.experimental import pallas as pl
from jax.experimental.pallas import tpu as pltpu
from jax.sharding import Mesh
from jax.sharding import PartitionSpec as P

beta_one = 0.9
beta_two = 0.95
bias_one = 1.0 - 0.9**10
bias_two = 1.0 - 0.95**10
rate = 0.001
decay = 0.1
eps_value = 1e-08

SH = 16384
N_DP = 64
PAIR = ("zl", "core")
DP = ("zh", "x", "y")
STRIDE = {"zh": 16, "x": 4, "y": 1}
MESH = pl.DeviceIdType.MESH

XYZ, YXZ, ZXY, ZYX = ("x", "y", "zh"), ("y", "x", "zh"), ("zh", "x", "y"), ("zh", "y", "x")
PARTS = (
    (ZXY, 12, 8, (2,)),
    (ZYX, 12, 8, (2,)),
    (XYZ, 28, 16, (2,)),
    (YXZ, 28, 16, (2,)),
    (XYZ, 12, 8, (1, 2)),
    (YXZ, 12, 8, (1, 2)),
    (XYZ, 12, 8, (1, 2)),
    (YXZ, 12, 8, (1, 2)),
)
START = tuple(sum(p[1] for p in PARTS[:i]) for i in range(len(PARTS)))
LATE = (6, 7,)
EARLY = 6
LOADING = (2, 3, 0, 1) + tuple(range(4, len(PARTS)))
ORDER_A = (2,3,4,5,0,1,6,7)
ORDER_SUM = (2,3,0,1,4,5,6,7)
ORDER_LATER = (2,3,0,1,4,5,6,7)
AP, AM, BP, BM, CP, CM = range(6)
RECV = [(i, phase, a) for i, p in enumerate(PARTS) for phase in range(3) for a in (True, False) if not (a and phase in p[3])]
RECV = {key: n for n, key in enumerate(RECV)}


def kernel(
    partner_hbm, w_hbm, m_hbm, v_hbm, g_hbm, state, squares_sum,
    stage, own, cand, grads, cand_g, near, far,
    gauge, partner, partner_sem, load_sem, own_sem, ring_send, ring_recv, rest_send, pair_recv, norm_recv, *ring_bufs,
):
    data = [ring_bufs[6 * p : 6 * p + 3] for p in range(len(PARTS))]
    landing = [ring_bufs[6 * p + 3 : 6 * p + 6] for p in range(len(PARTS))]
    at = {a: lax.axis_index(a) for a in PAIR + DP}

    def beside(axis, step):
        return lax.rem(at[axis] + step + 4, 4)

    groups = (2, 1, -1, 0)
    for i in groups:
        for zh in range(4):
            cols = pl.ds((zh * 16 + beside("x", i) * 4) * SH, 4 * SH)
            pltpu.make_async_copy(g_hbm.at[0, :, cols], stage.at[:, cols], load_sem.at[i % 4]).start()
    for i, ref in enumerate((w_hbm, m_hbm, v_hbm)):
        pltpu.make_async_copy(ref, own.at[i], own_sem).start()

    partner_copy = pltpu.make_async_copy(partner_hbm, partner, partner_sem)
    partner_copy.start()

    def loaded(i):
        part_of = stage.at[:, pl.ds(0, 16 * SH)]
        pltpu.make_async_copy(part_of, part_of, load_sem.at[i % 4]).wait()

    barrier = pltpu.get_barrier_semaphore()
    near_ids = [
        {"zh": beside("zh", k // 4), "zl": lax.rem(at["zl"] + (k // 2) % 2, 2), "core": lax.rem(at["core"] + k % 2, 2)}
        for k in range(16)
    ]
    far_ids = [{"x": beside("x", k // 4), "y": beside("y", k % 4)} for k in range(16)]
    for axis in DP:
        for step in (1, -1):
            pl.semaphore_signal(barrier, inc=1, device_id={axis: beside(axis, step)}, device_id_type=MESH)
    for axis in PAIR:
        pl.semaphore_signal(barrier, inc=1, device_id={axis: 1 - at[axis]}, device_id_type=MESH)

    def pieces(width):
        return [pl.ds(lo, min(1024, width - lo)) for lo in range(0, width, 1024)]

    def convert(part, c0, half):
        order, rows = PARTS[part][:2]
        dst = data[part][0]
        for c1 in (2 * half, 2 * half + 1):

            def body(c2, carry, c1=c1):
                block = c0 * STRIDE[order[0]] + c1 * STRIDE[order[1]] + c2 * STRIDE[order[2]]
                for p in pieces(rows * 128):
                    cols = pl.ds(pl.multiple_of(block * SH + START[part] * 128 + p.start, 128), p.size)
                    dst[c0, c1, c2, :, p] = stage[0:1, cols].astype(jnp.float32)
                return carry

            lax.fori_loop(0, 4, body, 0)

    def halves(part):
        rows, cut = PARTS[part][1:3]
        return pl.ds(0, cut * 128), pl.ds(cut * 128, (rows - cut) * 128)

    def view(part, phase, c, half):
        ref = data[part][phase]
        return ref.at[c, pl.ds(2 * half, 2)] if phase < 2 else ref.at[c, :, halves(part)[half]]

    def landed(part, phase, kind, half):
        ref = landing[part][phase].at[kind]
        return ref if phase < 2 else ref.at[:, pl.ds(0, halves(part)[half].size)]

    HALF = {AP: 0, AM: 1, BP: 1, BM: 0, CP: 0, CM: 1}
    CHUNK = {AP: 2, AM: -2, BP: 1, BM: -1, CP: 1, CM: -1}

    def ring(part, phase, kind):
        axis = PARTS[part][0][phase]
        return pltpu.make_async_remote_copy(
            src_ref=view(part, phase, beside(axis, CHUNK[kind]), HALF[kind]),
            dst_ref=landed(part, phase, kind, HALF[kind]),
            send_sem=ring_send,
            recv_sem=ring_recv.at[RECV[part, phase, kind < BP]],
            device_id={axis: beside(axis, 1 if kind in (AP, BP, CP) else -1)},
            device_id_type=MESH,
        )

    def wait_bytes(ref, sem):
        pltpu.make_async_copy(ref, ref, sem).wait()

    def add_up(dst, *srcs):
        lead, width = dst.shape[:-2], dst.shape[-1]

        def one(idx):
            for p in pieces(width):
                at_p = idx + (slice(None), p)
                total = srcs[0][at_p]
                for s in srcs[1:]:
                    total = total + s[at_p]
                dst[at_p] = total

        if len(lead) == 2:

            def body(i, carry):
                for j in range(lead[0]):
                    one((j, i))
                return carry

            lax.fori_loop(0, lead[1], body, 0)
        else:
            for j in range(lead[0] if lead else 1):
                one((j,) if lead else ())

    def straight(part, phase, step):
        axis = PARTS[part][0][phase]
        there = beside(axis, step)
        return pltpu.make_async_remote_copy(
            src_ref=data[part][phase].at[there],
            dst_ref=landing[part][phase].at[step - 1],
            send_sem=ring_send,
            recv_sem=ring_recv.at[RECV[part, phase, False]],
            device_id={axis: there},
            device_id_type=MESH,
        )

    def is_straight(part, phase):
        return phase in PARTS[part][3]

    def open_phase(part, phase):
        if is_straight(part, phase):
            for step in (2, 1, 3):
                straight(part, phase, step).start()
            return
        for kind in (AP, AM, BP, BM):
            ring(part, phase, kind).start()

    def forward(part, phase):
        if is_straight(part, phase):
            return
        axis = PARTS[part][0][phase]
        arrived = data[part][2].at[0] if phase == 2 else landing[part][phase].at[pl.ds(0, 2)]
        wait_bytes(arrived, ring_recv.at[RECV[part, phase, True]])
        for a, c in ((AP, CP), (AM, CM)):
            mine = view(part, phase, beside(axis, CHUNK[c]), HALF[c])
            add_up(mine, mine, landed(part, phase, a, HALF[a]))
            ring(part, phase, c).start()

    def close_phase(part, phase):
        axis = PARTS[part][0][phase]
        if is_straight(part, phase):
            arrived = landing[part][phase]
            wait_bytes(arrived, ring_recv.at[RECV[part, phase, False]])
            out = data[part][2] if phase == 1 else grads.at[:, pl.ds(START[part] * 128, PARTS[part][1] * 128)]
            add_up(out, data[part][phase].at[at[axis]], *[arrived.at[i] for i in range(3)])
            return
        last = data[part][2].at[pl.ds(0, 2)]
        wait_bytes(last if phase == 2 else landing[part][phase].at[pl.ds(2, 4)], ring_recv.at[RECV[part, phase, False]])
        for half, b, c in ((0, BM, CP), (1, BP, CM)):
            srcs = (
                view(part, phase, at[axis], half),
                landed(part, phase, b, half),
                landed(part, phase, c, half),
            )
            if phase < 2:
                add_up(data[part][phase + 1].at[pl.ds(2 * half, 2)], *srcs)
            else:
                cols = halves(part)[half]
                add_up(grads.at[:, pl.ds(START[part] * 128 + cols.start, cols.size)], *srcs)

    for n, part in enumerate(LOADING):
        axis = PARTS[part][0][0]
        for i in (groups[:1], groups[1:])[n] if n < 2 else ():
            loaded(i)
        convert(part, beside(axis, 2), 0)
        convert(part, beside(axis, 2), 1)
        if n == 0:
            pl.semaphore_wait(barrier, 8)
        ring(part, 0, AP).start()
        ring(part, 0, AM).start()
    for part in LOADING:
        axis = PARTS[part][0][0]
        convert(part, beside(axis, 1), 1)
        convert(part, beside(axis, -1), 0)
        if part in LATE:
            continue
        ring(part, 0, BP).start()
        ring(part, 0, BM).start()
    for part in LOADING:
        axis = PARTS[part][0][0]
        convert(part, beside(axis, 1), 0)
        convert(part, beside(axis, -1), 1)
    for part in ORDER_A:
        if part in LATE:
            ring(part, 0, BP).start()
            ring(part, 0, BM).start()
        forward(part, 0)
    for part in LOADING:
        axis = PARTS[part][0][0]
        convert(part, at[axis], 0)
        convert(part, at[axis], 1)

    def pair_copy(src, dst, n, axis):
        return pltpu.make_async_remote_copy(
            src_ref=src, dst_ref=dst, send_sem=rest_send, recv_sem=pair_recv.at[n],
            device_id={axis: 1 - at[axis]}, device_id_type=MESH,
        )

    wait_bytes(own, own_sem)
    shard_1 = pair_copy(own, cand.at[0], 0, "core")
    shard_2 = pair_copy(own, cand.at[2], 1, "zl")
    shard_3 = pair_copy(cand.at[2], cand.at[1], 0, "core")

    mine = at["zl"] * 2 + at["core"]
    partner_copy.wait()
    mate = partner[0, mine]
    apart = jnp.full((1, 1024), mine ^ mate, jnp.int32)
    is_one, is_two = apart == 1, apart == 2
    survive = jnp.full((1, 1024), mate - mine, jnp.int32) > 0

    def keep(a, cols, value, values):
        theirs = jnp.where(is_one, values[0], jnp.where(is_two, values[1], values[2]))
        state[a, 0:1, cols] = jnp.where(survive, value, 0.0)
        state[a, 1:2, cols] = jnp.where(survive, theirs, 0.0)

    def choose(i, carry):
        cols = pl.ds(pl.multiple_of(i * 1024, 1024), 1024)
        for a in range(3):
            keep(a, cols, own[a, :, cols], [cand[k, a, :, cols] for k in (0, 2, 1)])
        return carry

    def choose_grads(i, carry):
        cols = pl.ds(pl.multiple_of(i * 1024, 1024), 1024)
        keep(3, cols, grads[:, cols], [cand_g[k, :, cols] for k in (0, 2, 1)])
        return carry

    early = START[EARLY] * 128
    shares = (pl.ds(0, early), pl.ds(early, SH - early))

    def grads_copy(step, share):
        src = cand_g.at[2] if step == 2 else grads
        return pair_copy(
            src.at[:, shares[share]], cand_g.at[(0, 2, 1)[step], :, shares[share]], 2 + 2 * share + step % 2, ("core", "zl", "core")[step]
        )

    for phase in (0, 1, 2):
        for part in ORDER_LATER if phase else ORDER_SUM:
            close_phase(part, phase)
            if phase < 2:
                open_phase(part, phase + 1)
            elif part == [p for p in ORDER_LATER if p < EARLY][-1]:
                grads_copy(0, 0).start()
                grads_copy(1, 0).start()
            if phase == 0 and part == 1:
                shard_1.start()
                shard_2.start()
        if phase < 2:
            for part in ORDER_LATER:
                forward(part, phase + 1)
        if phase == 0:
            shard_2.wait_recv()
            shard_3.start()
        if phase == 1:
            wait_bytes(cand.at[pl.ds(0, 2)], pair_recv.at[0])
            lax.fori_loop(0, 16, choose, 0)

    def squares(i, total):
        tile = grads[:, pl.ds(i * 1024, 1024)]
        return total + tile * tile

    total = functools.reduce(lambda t, i: squares(i, t), range(16), jnp.zeros((1, 1024), jnp.float32))
    near[0] = jnp.sum(total.reshape(8, 128), axis=0, keepdims=True)

    def spread(buf, k, ids, n):
        return pltpu.make_async_remote_copy(
            src_ref=buf.at[0], dst_ref=buf.at[k], send_sem=rest_send, recv_sem=norm_recv.at[n],
            device_id=ids[k], device_id_type=MESH,
        )

    for k in sorted(range(1, 16), key=lambda k: -min(k // 4, 4 - k // 4)):
        spread(near, k, near_ids, 0).start()
    grads_copy(0, 1).start()
    grads_copy(1, 1).start()
    grads_copy(1, 0).wait_recv()
    grads_copy(2, 0).start()
    wait_bytes(near.at[pl.ds(1, 15)], norm_recv.at[0])
    far[0] = functools.reduce(jnp.add, [near[k] for k in range(16)])
    for k in sorted(range(1, 16), key=lambda k: -(min(k // 4, 4 - k // 4) + min(k % 4, 4 - k % 4))):
        spread(far, k, far_ids, 1).start()
    grads_copy(1, 1).wait_recv()
    grads_copy(2, 1).start()
    for share in (0, 1):
        wait_bytes(cand_g.at[pl.ds(0, 2), :, shares[share]], pair_recv.at[2 + 2 * share])
    lax.fori_loop(0, 16, choose_grads, 0)

    wait_bytes(gauge.at[:, pl.ds(0, 63 * SH)], ring_send)
    wait_bytes(gauge.at[:, pl.ds(0, 12 * SH + 30 * 128)], rest_send)
    wait_bytes(far.at[pl.ds(1, 15)], norm_recv.at[1])
    squares_sum[...] = functools.reduce(jnp.add, [far[k] for k in range(16)])


def update_kernel(state, squares_sum, out_w, out_m, out_v, buf, sem):
    norm2 = jnp.sum(squares_sum[...], axis=1, keepdims=True)
    scale = 1.0 / jnp.maximum(jnp.sqrt(norm2 / (4 * N_DP * SH)), 1.0)
    outs = (out_w, out_m, out_v)
    n = SH // 4

    def copies(q):
        cols = pl.ds(pl.multiple_of(q * n, n), n)
        return [pltpu.make_async_copy(buf.at[a, :, cols], outs[a].at[0, 0, :, cols], sem.at[a]) for a in range(3)]

    def quarter(q, carry):
        for i in range(n // 512):
            cols = pl.ds(pl.multiple_of(q * n + i * 512, 512), 512)
            weights, first, second, total = [state[a, :, cols] for a in range(4)]
            scaled = scale * total
            first_new = beta_one * first + (1.0 - beta_one) * scaled
            second_new = beta_two * second + (1.0 - beta_two) * scaled * scaled
            change = first_new * (1.0 / bias_one) / (jnp.sqrt(second_new * (1.0 / bias_two)) + eps_value) + decay * weights
            buf[0, :, cols] = weights - rate * change
            buf[1, :, cols] = first_new
            buf[2, :, cols] = second_new
        for c in copies(q):
            c.start()
        return carry

    lax.fori_loop(0, 4, quarter, 0)
    for a in range(3):
        pltpu.make_async_copy(buf.at[a], outs[a].at[0, 0], sem.at[a]).wait()


def on_device(master, moment1, moment2, local_grad, partner):
    f32 = jnp.float32
    vmem = []
    for _, rows, cut, straight in PARTS:
        vmem += [pltpu.VMEM(n + (1, rows * 128), f32) for n in ((4, 4, 4), (4, 4), (4,), (6, 2, 4), (3, 4) if 1 in straight else (6, 2))]
        vmem.append(pltpu.VMEM((3, 1, rows * 128) if 2 in straight else (6, 1, max(cut, rows - cut) * 128), f32))
    dma = pltpu.SemaphoreType.DMA
    out = jax.ShapeDtypeStruct((1, 1, 2, SH), f32)
    state, squares_sum = pl.pallas_call(
        kernel,
        out_shape=(pltpu.VMEM((4, 2, SH), f32), pltpu.VMEM((1, 128), f32)),
        in_specs=[pl.BlockSpec(memory_space=pltpu.HBM)] * 5,
        out_specs=[pl.BlockSpec(memory_space=pltpu.VMEM)] * 2,
        scratch_shapes=[
            pltpu.VMEM((1, N_DP * SH), jnp.bfloat16),
            pltpu.VMEM((3, 1, SH), f32),
            pltpu.VMEM((3, 3, 1, SH), f32),
            pltpu.VMEM((1, SH), f32),
            pltpu.VMEM((3, 1, SH), f32),
            pltpu.VMEM((16, 1, 128), f32),
            pltpu.VMEM((16, 1, 128), f32),
            pltpu.VMEM((1, 63 * SH), f32),
        ]
        + [pltpu.SMEM((1, 4), jnp.int32), dma]
        + [dma((4,)), dma, dma, dma((len(RECV),)), dma, dma((6,)), dma((2,))]
        + vmem,
        compiler_params=pltpu.CompilerParams(collective_id=0, has_side_effects=True),
        name="step",
    )(partner, master, moment1, moment2, local_grad)
    return pl.pallas_call(
        update_kernel,
        out_shape=(out, out, out),
        in_specs=[pl.BlockSpec(memory_space=pltpu.VMEM)] * 2,
        out_specs=[pl.BlockSpec(memory_space=pltpu.HBM)] * 3,
        scratch_shapes=[pltpu.VMEM((3, 2, SH), f32), dma((3,))],
        name="update",
    )(*[pltpu.with_memory_space_constraint(v, pltpu.VMEM) for v in (state, squares_sum)])


def solution(mesh):
    finer = Mesh(mesh.devices.reshape(2, 2, 4, 4, 4), PAIR + DP)
    in_specs = (P(PAIR, DP), P(PAIR, DP), P(PAIR, DP), P(PAIR, DP, None), P(DP, None))
    out_specs = (P(PAIR, DP, None, None),) * 3
    return jax.shard_map(on_device, mesh=finer, in_specs=in_specs, out_specs=out_specs, check_vma=False)
```

```python
import functools

import jax
import jax.numpy as jnp
from jax import lax
from jax.experimental import pallas as pl
from jax.experimental.pallas import tpu as pltpu
from jax.sharding import Mesh
from jax.sharding import PartitionSpec as P

beta_one = 0.9
beta_two = 0.95
bias_one = 1.0 - 0.9**10
bias_two = 1.0 - 0.95**10
rate = 0.001
decay = 0.1
eps_value = 1e-08

SH = 16384
N_DP = 64
PAIR = ("zl", "core")
DP = ("zh", "x", "y")
STRIDE = {"zh": 16, "x": 4, "y": 1}
MESH = pl.DeviceIdType.MESH

XYZ, YXZ, ZXY, ZYX = ("x", "y", "zh"), ("y", "x", "zh"), ("zh", "x", "y"), ("zh", "y", "x")
PARTS = (
    (ZXY, 12, 8, (2,)),
    (ZYX, 12, 8, (2,)),
    (XYZ, 28, 16, (2,)),
    (YXZ, 28, 16, (2,)),
    (XYZ, 12, 8, (1, 2)),
    (YXZ, 12, 8, (1, 2)),
    (XYZ, 12, 8, (1, 2)),
    (YXZ, 12, 8, (1, 2)),
)
START = tuple(sum(p[1] for p in PARTS[:i]) for i in range(len(PARTS)))
LATE = (6, 7,)
EARLY = 4
LOADING = (2, 3, 0, 1) + tuple(range(4, len(PARTS)))
ORDER_A = (2,3,4,5,0,1,6,7)
ORDER_SUM = (2,3,0,1,4,5,6,7)
ORDER_LATER = (2,3,0,1,4,5,6,7)
AP, AM, BP, BM, CP, CM = range(6)
RECV = [(i, phase, a) for i, p in enumerate(PARTS) for phase in range(3) for a in (True, False) if not (a and phase in p[3])]
RECV = {key: n for n, key in enumerate(RECV)}


def kernel(
    partner_hbm, w_hbm, m_hbm, v_hbm, g_hbm, state, squares_sum,
    stage, own, cand, grads, cand_g, near, far,
    gauge, partner, partner_sem, load_sem, own_sem, ring_send, ring_recv, rest_send, pair_recv, norm_recv, *ring_bufs,
):
    data = [ring_bufs[6 * p : 6 * p + 3] for p in range(len(PARTS))]
    landing = [ring_bufs[6 * p + 3 : 6 * p + 6] for p in range(len(PARTS))]
    at = {a: lax.axis_index(a) for a in PAIR + DP}

    def beside(axis, step):
        return lax.rem(at[axis] + step + 4, 4)

    groups = (2, 1, -1, 0)
    for i in groups:
        for zh in range(4):
            cols = pl.ds((zh * 16 + beside("x", i) * 4) * SH, 4 * SH)
            pltpu.make_async_copy(g_hbm.at[0, :, cols], stage.at[:, cols], load_sem.at[i % 4]).start()
    for i, ref in enumerate((w_hbm, m_hbm, v_hbm)):
        pltpu.make_async_copy(ref, own.at[i], own_sem).start()

    partner_copy = pltpu.make_async_copy(partner_hbm, partner, partner_sem)
    partner_copy.start()

    def loaded(i):
        part_of = stage.at[:, pl.ds(0, 16 * SH)]
        pltpu.make_async_copy(part_of, part_of, load_sem.at[i % 4]).wait()

    barrier = pltpu.get_barrier_semaphore()
    near_ids = [
        {"zh": beside("zh", k // 4), "zl": lax.rem(at["zl"] + (k // 2) % 2, 2), "core": lax.rem(at["core"] + k % 2, 2)}
        for k in range(16)
    ]
    far_ids = [{"x": beside("x", k // 4), "y": beside("y", k % 4)} for k in range(16)]
    for axis in DP:
        for step in (1, -1):
            pl.semaphore_signal(barrier, inc=1, device_id={axis: beside(axis, step)}, device_id_type=MESH)
    for axis in PAIR:
        pl.semaphore_signal(barrier, inc=1, device_id={axis: 1 - at[axis]}, device_id_type=MESH)

    def pieces(width):
        return [pl.ds(lo, min(1024, width - lo)) for lo in range(0, width, 1024)]

    def convert(part, c0, half):
        order, rows = PARTS[part][:2]
        dst = data[part][0]
        for c1 in (2 * half, 2 * half + 1):

            def body(c2, carry, c1=c1):
                block = c0 * STRIDE[order[0]] + c1 * STRIDE[order[1]] + c2 * STRIDE[order[2]]
                for p in pieces(rows * 128):
                    cols = pl.ds(pl.multiple_of(block * SH + START[part] * 128 + p.start, 128), p.size)
                    dst[c0, c1, c2, :, p] = stage[0:1, cols].astype(jnp.float32)
                return carry

            lax.fori_loop(0, 4, body, 0)

    def halves(part):
        rows, cut = PARTS[part][1:3]
        return pl.ds(0, cut * 128), pl.ds(cut * 128, (rows - cut) * 128)

    def view(part, phase, c, half):
        ref = data[part][phase]
        return ref.at[c, pl.ds(2 * half, 2)] if phase < 2 else ref.at[c, :, halves(part)[half]]

    def landed(part, phase, kind, half):
        ref = landing[part][phase].at[kind]
        return ref if phase < 2 else ref.at[:, pl.ds(0, halves(part)[half].size)]

    HALF = {AP: 0, AM: 1, BP: 1, BM: 0, CP: 0, CM: 1}
    CHUNK = {AP: 2, AM: -2, BP: 1, BM: -1, CP: 1, CM: -1}

    def ring(part, phase, kind):
        axis = PARTS[part][0][phase]
        return pltpu.make_async_remote_copy(
            src_ref=view(part, phase, beside(axis, CHUNK[kind]), HALF[kind]),
            dst_ref=landed(part, phase, kind, HALF[kind]),
            send_sem=ring_send,
            recv_sem=ring_recv.at[RECV[part, phase, kind < BP]],
            device_id={axis: beside(axis, 1 if kind in (AP, BP, CP) else -1)},
            device_id_type=MESH,
        )

    def wait_bytes(ref, sem):
        pltpu.make_async_copy(ref, ref, sem).wait()

    def add_up(dst, *srcs):
        lead, width = dst.shape[:-2], dst.shape[-1]

        def one(idx):
            for p in pieces(width):
                at_p = idx + (slice(None), p)
                total = srcs[0][at_p]
                for s in srcs[1:]:
                    total = total + s[at_p]
                dst[at_p] = total

        if len(lead) == 2:

            def body(i, carry):
                for j in range(lead[0]):
                    one((j, i))
                return carry

            lax.fori_loop(0, lead[1], body, 0)
        else:
            for j in range(lead[0] if lead else 1):
                one((j,) if lead else ())

    def straight(part, phase, step):
        axis = PARTS[part][0][phase]
        there = beside(axis, step)
        return pltpu.make_async_remote_copy(
            src_ref=data[part][phase].at[there],
            dst_ref=landing[part][phase].at[step - 1],
            send_sem=ring_send,
            recv_sem=ring_recv.at[RECV[part, phase, False]],
            device_id={axis: there},
            device_id_type=MESH,
        )

    def is_straight(part, phase):
        return phase in PARTS[part][3]

    def open_phase(part, phase):
        if is_straight(part, phase):
            for step in (2, 1, 3):
                straight(part, phase, step).start()
            return
        for kind in (AP, AM, BP, BM):
            ring(part, phase, kind).start()

    def forward(part, phase):
        if is_straight(part, phase):
            return
        axis = PARTS[part][0][phase]
        arrived = data[part][2].at[0] if phase == 2 else landing[part][phase].at[pl.ds(0, 2)]
        wait_bytes(arrived, ring_recv.at[RECV[part, phase, True]])
        for a, c in ((AP, CP), (AM, CM)):
            mine = view(part, phase, beside(axis, CHUNK[c]), HALF[c])
            add_up(mine, mine, landed(part, phase, a, HALF[a]))
            ring(part, phase, c).start()

    def close_phase(part, phase):
        axis = PARTS[part][0][phase]
        if is_straight(part, phase):
            arrived = landing[part][phase]
            wait_bytes(arrived, ring_recv.at[RECV[part, phase, False]])
            out = data[part][2] if phase == 1 else grads.at[:, pl.ds(START[part] * 128, PARTS[part][1] * 128)]
            add_up(out, data[part][phase].at[at[axis]], *[arrived.at[i] for i in range(3)])
            return
        last = data[part][2].at[pl.ds(0, 2)]
        wait_bytes(last if phase == 2 else landing[part][phase].at[pl.ds(2, 4)], ring_recv.at[RECV[part, phase, False]])
        for half, b, c in ((0, BM, CP), (1, BP, CM)):
            srcs = (
                view(part, phase, at[axis], half),
                landed(part, phase, b, half),
                landed(part, phase, c, half),
            )
            if phase < 2:
                add_up(data[part][phase + 1].at[pl.ds(2 * half, 2)], *srcs)
            else:
                cols = halves(part)[half]
                add_up(grads.at[:, pl.ds(START[part] * 128 + cols.start, cols.size)], *srcs)

    for n, part in enumerate(LOADING):
        axis = PARTS[part][0][0]
        for i in (groups[:1], groups[1:])[n] if n < 2 else ():
            loaded(i)
        convert(part, beside(axis, 2), 0)
        convert(part, beside(axis, 2), 1)
        if n == 0:
            pl.semaphore_wait(barrier, 8)
        ring(part, 0, AP).start()
        ring(part, 0, AM).start()
    for part in LOADING:
        axis = PARTS[part][0][0]
        convert(part, beside(axis, 1), 1)
        convert(part, beside(axis, -1), 0)
        if part in LATE:
            continue
        ring(part, 0, BP).start()
        ring(part, 0, BM).start()
    for part in LOADING:
        axis = PARTS[part][0][0]
        convert(part, beside(axis, 1), 0)
        convert(part, beside(axis, -1), 1)
    for part in ORDER_A:
        if part in LATE:
            ring(part, 0, BP).start()
            ring(part, 0, BM).start()
        forward(part, 0)
    for part in LOADING:
        axis = PARTS[part][0][0]
        convert(part, at[axis], 0)
        convert(part, at[axis], 1)

    def pair_copy(src, dst, n, axis):
        return pltpu.make_async_remote_copy(
            src_ref=src, dst_ref=dst, send_sem=rest_send, recv_sem=pair_recv.at[n],
            device_id={axis: 1 - at[axis]}, device_id_type=MESH,
        )

    wait_bytes(own, own_sem)
    shard_1 = pair_copy(own, cand.at[0], 0, "core")
    shard_2 = pair_copy(own, cand.at[2], 1, "zl")
    shard_3 = pair_copy(cand.at[2], cand.at[1], 0, "core")

    mine = at["zl"] * 2 + at["core"]
    partner_copy.wait()
    mate = partner[0, mine]
    apart = jnp.full((1, 1024), mine ^ mate, jnp.int32)
    is_one, is_two = apart == 1, apart == 2
    survive = jnp.full((1, 1024), mate - mine, jnp.int32) > 0

    def keep(a, cols, value, values):
        theirs = jnp.where(is_one, values[0], jnp.where(is_two, values[1], values[2]))
        state[a, 0:1, cols] = jnp.where(survive, value, 0.0)
        state[a, 1:2, cols] = jnp.where(survive, theirs, 0.0)

    def choose(i, carry):
        cols = pl.ds(pl.multiple_of(i * 1024, 1024), 1024)
        for a in range(3):
            keep(a, cols, own[a, :, cols], [cand[k, a, :, cols] for k in (0, 2, 1)])
        return carry

    def choose_grads(i, carry):
        cols = pl.ds(pl.multiple_of(i * 1024, 1024), 1024)
        keep(3, cols, grads[:, cols], [cand_g[k, :, cols] for k in (0, 2, 1)])
        return carry

    early = START[EARLY] * 128
    shares = (pl.ds(0, early), pl.ds(early, SH - early))

    def grads_copy(step, share):
        src = cand_g.at[2] if step == 2 else grads
        return pair_copy(
            src.at[:, shares[share]], cand_g.at[(0, 2, 1)[step], :, shares[share]], 2 + 2 * share + step % 2, ("core", "zl", "core")[step]
        )

    for phase in (0, 1, 2):
        for part in ORDER_LATER if phase else ORDER_SUM:
            close_phase(part, phase)
            if phase < 2:
                open_phase(part, phase + 1)
            elif part == [p for p in ORDER_LATER if p < EARLY][-1]:
                grads_copy(0, 0).start()
                grads_copy(1, 0).start()
            if phase == 0 and part == 1:
                shard_1.start()
                shard_2.start()
        if phase < 2:
            for part in ORDER_LATER:
                forward(part, phase + 1)
        if phase == 0:
            shard_2.wait_recv()
            shard_3.start()
        if phase == 1:
            wait_bytes(cand.at[pl.ds(0, 2)], pair_recv.at[0])
            lax.fori_loop(0, 16, choose, 0)

    def squares(i, total):
        tile = grads[:, pl.ds(i * 1024, 1024)]
        return total + tile * tile

    total = functools.reduce(lambda t, i: squares(i, t), range(16), jnp.zeros((1, 1024), jnp.float32))
    near[0] = jnp.sum(total.reshape(8, 128), axis=0, keepdims=True)

    def spread(buf, k, ids, n):
        return pltpu.make_async_remote_copy(
            src_ref=buf.at[0], dst_ref=buf.at[k], send_sem=rest_send, recv_sem=norm_recv.at[n],
            device_id=ids[k], device_id_type=MESH,
        )

    for k in sorted(range(1, 16), key=lambda k: -min(k // 4, 4 - k // 4)):
        spread(near, k, near_ids, 0).start()
    grads_copy(0, 1).start()
    grads_copy(1, 1).start()
    grads_copy(1, 0).wait_recv()
    grads_copy(2, 0).start()
    wait_bytes(near.at[pl.ds(1, 15)], norm_recv.at[0])
    far[0] = functools.reduce(jnp.add, [near[k] for k in range(16)])
    for k in sorted(range(1, 16), key=lambda k: -(min(k // 4, 4 - k // 4) + min(k % 4, 4 - k % 4))):
        spread(far, k, far_ids, 1).start()
    grads_copy(1, 1).wait_recv()
    grads_copy(2, 1).start()
    for share in (0, 1):
        wait_bytes(cand_g.at[pl.ds(0, 2), :, shares[share]], pair_recv.at[2 + 2 * share])
    lax.fori_loop(0, 16, choose_grads, 0)

    wait_bytes(gauge.at[:, pl.ds(0, 63 * SH)], ring_send)
    wait_bytes(gauge.at[:, pl.ds(0, 12 * SH + 30 * 128)], rest_send)
    wait_bytes(far.at[pl.ds(1, 15)], norm_recv.at[1])
    squares_sum[...] = functools.reduce(jnp.add, [far[k] for k in range(16)])


def update_kernel(state, squares_sum, out_w, out_m, out_v, buf, sem):
    norm2 = jnp.sum(squares_sum[...], axis=1, keepdims=True)
    scale = 1.0 / jnp.maximum(jnp.sqrt(norm2 / (4 * N_DP * SH)), 1.0)
    outs = (out_w, out_m, out_v)
    n = SH // 4

    def copies(q):
        cols = pl.ds(pl.multiple_of(q * n, n), n)
        return [pltpu.make_async_copy(buf.at[a, :, cols], outs[a].at[0, 0, :, cols], sem.at[a]) for a in range(3)]

    def quarter(q, carry):
        for i in range(n // 512):
            cols = pl.ds(pl.multiple_of(q * n + i * 512, 512), 512)
            weights, first, second, total = [state[a, :, cols] for a in range(4)]
            scaled = scale * total
            first_new = beta_one * first + (1.0 - beta_one) * scaled
            second_new = beta_two * second + (1.0 - beta_two) * scaled * scaled
            change = first_new * (1.0 / bias_one) / (jnp.sqrt(second_new * (1.0 / bias_two)) + eps_value) + decay * weights
            buf[0, :, cols] = weights - rate * change
            buf[1, :, cols] = first_new
            buf[2, :, cols] = second_new
        for c in copies(q):
            c.start()
        return carry

    lax.fori_loop(0, 4, quarter, 0)
    for a in range(3):
        pltpu.make_async_copy(buf.at[a], outs[a].at[0, 0], sem.at[a]).wait()


def on_device(master, moment1, moment2, local_grad, partner):
    f32 = jnp.float32
    vmem = []
    for _, rows, cut, straight in PARTS:
        vmem += [pltpu.VMEM(n + (1, rows * 128), f32) for n in ((4, 4, 4), (4, 4), (4,), (6, 2, 4), (3, 4) if 1 in straight else (6, 2))]
        vmem.append(pltpu.VMEM((3, 1, rows * 128) if 2 in straight else (6, 1, max(cut, rows - cut) * 128), f32))
    dma = pltpu.SemaphoreType.DMA
    out = jax.ShapeDtypeStruct((1, 1, 2, SH), f32)
    state, squares_sum = pl.pallas_call(
        kernel,
        out_shape=(pltpu.VMEM((4, 2, SH), f32), pltpu.VMEM((1, 128), f32)),
        in_specs=[pl.BlockSpec(memory_space=pltpu.HBM)] * 5,
        out_specs=[pl.BlockSpec(memory_space=pltpu.VMEM)] * 2,
        scratch_shapes=[
            pltpu.VMEM((1, N_DP * SH), jnp.bfloat16),
            pltpu.VMEM((3, 1, SH), f32),
            pltpu.VMEM((3, 3, 1, SH), f32),
            pltpu.VMEM((1, SH), f32),
            pltpu.VMEM((3, 1, SH), f32),
            pltpu.VMEM((16, 1, 128), f32),
            pltpu.VMEM((16, 1, 128), f32),
            pltpu.VMEM((1, 63 * SH), f32),
        ]
        + [pltpu.SMEM((1, 4), jnp.int32), dma]
        + [dma((4,)), dma, dma, dma((len(RECV),)), dma, dma((6,)), dma((2,))]
        + vmem,
        compiler_params=pltpu.CompilerParams(collective_id=0, has_side_effects=True),
        name="step",
    )(partner, master, moment1, moment2, local_grad)
    return pl.pallas_call(
        update_kernel,
        out_shape=(out, out, out),
        in_specs=[pl.BlockSpec(memory_space=pltpu.VMEM)] * 2,
        out_specs=[pl.BlockSpec(memory_space=pltpu.HBM)] * 3,
        scratch_shapes=[pltpu.VMEM((3, 2, SH), f32), dma((3,))],
        name="update",
    )(*[pltpu.with_memory_space_constraint(v, pltpu.VMEM) for v in (state, squares_sum)])


def solution(mesh):
    finer = Mesh(mesh.devices.reshape(2, 2, 4, 4, 4), PAIR + DP)
    in_specs = (P(PAIR, DP), P(PAIR, DP), P(PAIR, DP), P(PAIR, DP, None), P(DP, None))
    out_specs = (P(PAIR, DP, None, None),) * 3
    return jax.shard_map(on_device, mesh=finer, in_specs=in_specs, out_specs=out_specs, check_vma=False)
```
